128 devices in a mesh: side: 2 (over y_lo), gx: 8 (over x, core), gy: 8 (over z, y_hi).
Axes of the slice: x: 4, y: 4 (y_hi: 2, y_lo: 2; y = y_hi * 2 + y_lo), z: 4, core: 2. Of those that a mesh axis runs over, the one named last changes fastest.
Arguments:
- populations: float32 [2, 19, 4, 256, 1024], P('side', None, None, 'gx', 'gy'), may hold values from 0.01 to 0.84, as said below
- solid_mask: int32 [2, 4, 256, 1024], P('side', None, 'gx', 'gy'), may hold values 0 or 1
- water_sheet: float32 [32, 256, 1024], P(None, 'gx', ('side', 'gy')), may hold values from 2 to 12
- current: float32 [256, 1024], P('gx', ('side', 'gy')), may hold values from 0.5 to 3
Outputs:
- populations_out: float32 [2, 19, 4, 256, 1024], P('side', None, None, 'gx', 'gy')
- sheet_out: float32 [32, 256, 1024], P(None, 'gx', ('side', 'gy'))
The draws below stay inside these ranges and needn't reach their ends.
Inputs may be any that keep to these rules, and one draw needn't show every extreme that they name: `populations`: every population is positive.
All inputs are finite; a program needn't handle non-finite values. No bound on the sum of `solid_mask` on one device may be relied on, other than what follows from the above.
Results may differ from the reference program's by a relative error of at most 0.0003.
Values sent between devices are 32-bit elements; how exact they have to be, the bound alone decides.
A program may use at most 64 MiB of HBM per device.

```python
import jax
import jax.numpy as jnp

LAYERS = 4
MEMBRANE = 32
STEPS = 8
SUBSTEPS = 2
NX = 256
NY = 1024
N_GY = 8


def draw_populations(key, part):
    weights = jnp.array((1.0 / 3.0,) + (1.0 / 18.0,) * 6 + (1.0 / 36.0,) * 12, jnp.float32)
    density_key = jax.random.fold_in(key, 11)
    noise_key = jax.random.fold_in(key, 23)
    log_density = jax.random.uniform(density_key, (2, 1, LAYERS, NX, NY), jnp.float32, jnp.log(0.5), jnp.log(2.0))
    noise = 0.2 * jax.random.uniform(noise_key, (2, 19, LAYERS, NX, NY), jnp.float32, -1.0, 1.0)
    return weights[None, :, None, None, None] * jnp.exp(log_density) * (1.0 + noise)


def with_ends(values, key, least, largest):
    longest = values.shape.index(max(values.shape))
    spots = []
    for shift in (0, 1):
        where = [jax.random.randint(jax.random.fold_in(key, axis), (), 0, length) for axis, length in enumerate(values.shape)]
        where[longest] = (where[longest] + shift) % values.shape[longest]
        spots.append(tuple(where))
    return values.at[spots[0]].set(least).at[spots[1]].set(largest)


def level_of(own_key, dims, pieces, low, high):
    def one(axis_at, shards_of):
        heights = jax.random.uniform(jax.random.fold_in(jax.random.fold_in(own_key, 6), axis_at), (shards_of,), jnp.float32, low / len(pieces), high / len(pieces))
        return jnp.repeat(jnp.exp(heights), dims[axis_at] // shards_of).reshape((-1,) + (1,) * (len(dims) - axis_at - 1))

    loudness = one(*pieces[0])
    for cut in pieces[1:]:
        loudness = loudness * one(*cut)
    return loudness


def setup_inputs(seed: int = 0) -> dict:
    splits = jax.random.split(jax.random.key(seed), 5)
    return {
        "populations": draw_populations(jax.random.fold_in(splits[4], 71), 0),
        "solid_mask": with_ends((jax.random.randint(splits[1], (2, LAYERS, NX, NY), 0, 4) < 3).astype(jnp.int32), jax.random.fold_in(splits[1], 1), 0, 1),
        "water_sheet": jnp.clip(2.0 + 10.0 * jax.random.uniform(splits[2], (MEMBRANE, NX, NY), jnp.float32) ** level_of(splits[2], (MEMBRANE, NX, NY), ((1, 8), (2, 16)), -0.2, 0.2), 2.0, 12.0),
        "current": jnp.clip(0.5 + 2.5 * jax.random.uniform(splits[3], (NX, NY), jnp.float32) ** level_of(splits[3], (NX, NY), ((0, 8), (1, 16)), -0.2, 0.2), 0.5, 3.0),
    }


velocity_table = ((0, 0, 0), (1, 0, 0), (-1, 0, 0), (0, 1, 0), (0, -1, 0), (0, 0, 1), (0, 0, -1),
                  (1, 1, 0), (-1, -1, 0), (1, -1, 0), (-1, 1, 0), (1, 0, 1), (-1, 0, -1),
                  (1, 0, -1), (-1, 0, 1), (0, 1, 1), (0, -1, -1), (0, 1, -1), (0, -1, 1))
opposite_index = (0, 2, 1, 4, 3, 6, 5, 8, 7, 10, 9, 12, 11, 14, 13, 16, 15, 18, 17)
weight_table = (1.0 / 3.0,) + (1.0 / 18.0,) * 6 + (1.0 / 36.0,) * 12
relax_time = 0.8
coupling = -3.0
wall_potential = 0.4
uptake_rate = 0.02
drag_rate = 0.03
base_diffusion = 0.05
slope_diffusion = 0.015


def density(fields):
    summed = fields[0]
    for direction in range(1, 19):
        summed = summed + fields[direction]
    return summed


def potential(density_now, solids):
    return jnp.where(solids > 0, 1.0 - jnp.exp(-density_now), wall_potential)


def attraction(padded):
    layers = padded.shape[0]
    inner_rows = padded.shape[1] - 2
    inner_cols = padded.shape[2] - 2
    zeros_layer = jnp.zeros((1,) + padded.shape[1:], jnp.float32)
    stacked = jnp.concatenate([zeros_layer, padded, zeros_layer], axis=0)
    totals = [None, None, None]
    for direction in range(1, 19):
        shift_x, shift_y, shift_z = velocity_table[direction]
        weighted = weight_table[direction] * stacked[1 + shift_z:1 + shift_z + layers,
                                                     1 + shift_x:1 + shift_x + inner_rows,
                                                     1 + shift_y:1 + shift_y + inner_cols]
        for component in range(3):
            factor = velocity_table[direction][component]
            if factor != 0:
                contribution = factor * weighted
                totals[component] = contribution if totals[component] is None else totals[component] + contribution
    centre = padded[:, 1:-1, 1:-1]
    return [-coupling * centre * summed for summed in totals]


def relax(fields, density_now, solids, padded):
    forces = attraction(padded)
    velocity = []
    for component in range(3):
        moment = None
        for direction in range(1, 19):
            factor = velocity_table[direction][component]
            if factor != 0:
                contribution = factor * fields[direction]
                moment = contribution if moment is None else moment + contribution
        velocity.append((moment + relax_time * forces[component]) / density_now)
    speed_squared = velocity[0] * velocity[0] + velocity[1] * velocity[1] + velocity[2] * velocity[2]
    is_pore = solids > 0
    relaxed = []
    for direction in range(19):
        projected = jnp.zeros_like(density_now)
        for component in range(3):
            factor = velocity_table[direction][component]
            if factor != 0:
                projected = projected + factor * velocity[component]
        balance = weight_table[direction] * density_now * (
            1.0 + 3.0 * projected + 4.5 * projected * projected - 1.5 * speed_squared)
        collided = fields[direction] - (fields[direction] - balance) / relax_time
        relaxed.append(jnp.where(is_pore, collided, fields[opposite_index[direction]]))
    return jnp.stack(relaxed)


def propagate(padded, membrane_flux):
    inner_rows = padded.shape[2] - 2
    inner_cols = padded.shape[3] - 2
    centre = padded[:, :, 1:-1, 1:-1]
    result = []
    for direction in range(19):
        shift_x, shift_y, shift_z = velocity_table[direction]
        moved = padded[direction, :, 1 - shift_x:1 - shift_x + inner_rows, 1 - shift_y:1 - shift_y + inner_cols]
        if shift_z == 1:
            inflow = centre[opposite_index[direction], :1] - 6.0 * weight_table[direction] * membrane_flux[None]
            moved = jnp.concatenate([inflow, moved[:-1]], axis=0)
        elif shift_z == -1:
            moved = jnp.concatenate([moved[1:], centre[opposite_index[direction], -1:]], axis=0)
        result.append(moved)
    return jnp.stack(result)


def uptake(density_row):
    activity = density_row / (1.0 + density_row)
    return 0.043 + activity * (17.18 + activity * (-39.85 + 36.0 * activity))


def sheet_substep(water, current_rows, inflow_anode, inflow_cathode):
    diffusivity = base_diffusion + slope_diffusion * water
    face_z = -0.5 * (diffusivity[1:] + diffusivity[:-1]) * (water[1:] - water[:-1]) + drag_rate * current_rows[None] * water[:-1]
    change = jnp.concatenate([inflow_anode[None], face_z]) - jnp.concatenate([face_z, -inflow_cathode[None]])
    return water + change


def reference(populations, solid_mask, water_sheet, current):
    groups = 2 * N_GY
    sub_width = NY // (groups * N_GY)

    def to_sheet(field):
        return field.reshape(NX, N_GY, groups, sub_width).transpose(0, 2, 1, 3).reshape(NX, NY)

    def from_sheet(field):
        return field.reshape(NX, groups, N_GY, sub_width).transpose(0, 2, 1, 3).reshape(NX, NY)

    surface_anode = to_sheet(density(populations[0][:, :1])[0])
    surface_cathode = to_sheet(density(populations[1][:, :1])[0])
    inflow_anode = uptake_rate * (uptake(surface_anode) - water_sheet[0])
    inflow_cathode = uptake_rate * (uptake(surface_cathode) - water_sheet[-1])
    water = water_sheet
    for repeat in range(SUBSTEPS):
        water = sheet_substep(water, current, inflow_anode, inflow_cathode)
    results = []
    for which_side, inflow in ((0, inflow_anode), (1, inflow_cathode)):
        membrane_flux = from_sheet(inflow)
        lattice = populations[which_side]
        solids = solid_mask[which_side]
        for repeat in range(STEPS):
            density_now = density(lattice)
            padded = jnp.pad(potential(density_now, solids), ((0, 0), (1, 1), (1, 1)), mode="wrap")
            relaxed = relax(lattice, density_now, solids, padded)
            lattice = propagate(jnp.pad(relaxed, ((0, 0), (0, 0), (1, 1), (1, 1)), mode="wrap"), membrane_flux)
        results.append(lattice)
    return jnp.stack(results), water
```

```python
import functools

import jax
import jax.numpy as jnp
from jax import lax
from jax.experimental import pallas as pl
from jax.experimental.pallas import tpu as pltpu
from jax.sharding import PartitionSpec as P

STEPS = 8
SUBSTEPS = 2
LATTICE = 19
MESH = pl.DeviceIdType.MESH

velocity_table = (
    (0, 0, 0),
    (1, 0, 0),
    (-1, 0, 0),
    (0, 1, 0),
    (0, -1, 0),
    (0, 0, 1),
    (0, 0, -1),
    (1, 1, 0),
    (-1, -1, 0),
    (1, -1, 0),
    (-1, 1, 0),
    (1, 0, 1),
    (-1, 0, -1),
    (1, 0, -1),
    (-1, 0, 1),
    (0, 1, 1),
    (0, -1, -1),
    (0, 1, -1),
    (0, -1, 1),
)
opposite_index = (0, 2, 1, 4, 3, 6, 5, 8, 7, 10, 9, 12, 11, 14, 13, 16, 15, 18, 17)
weight_table = (1.0 / 3.0,) + (1.0 / 18.0,) * 6 + (1.0 / 36.0,) * 12
relax_time = 0.8
coupling = -3.0
wall_potential = 0.4
uptake_rate = 0.02
drag_rate = 0.03
base_diffusion = 0.05
slope_diffusion = 0.015

PAIRS = 10
PAD = 8
ROWS = 16 * PAIRS + 2 * PAD
MASK_PLANE = LATTICE
FLUX_PLANE = LATTICE + 1
PLANES = LATTICE + 2
RATE = 1.0 / relax_time
KAPPA = RATE / 36.0


def roll(values, shift):
    shift = shift % 128
    if shift == 0:
        return values
    return pltpu.roll(values, shift, values.ndim - 1)


def lanes_of(shape):
    return lax.broadcasted_iota(jnp.int32, shape, len(shape) - 1)


def uptake(density_row):
    activity = density_row / (1.0 + density_row)
    return 0.043 + activity * (17.18 + activity * (-39.85 + 36.0 * activity))


def pack_columns(ref, offset, rows):
    lanes = lanes_of((rows, 128))
    packed = None
    for m in range(4):
        part = roll(ref[pl.ds(m, rows, stride=4), :], 32 * m - offset)
        packed = part if packed is None else jnp.where(lanes >= 32 * m, part, packed)
    return packed


def unpack_columns(packed, ref):
    for m in range(4):
        ref[pl.ds(m, packed.shape[0], stride=4), :] = roll(packed, -32 * m)


def pack_pair(a, b):
    lower = lanes_of(a.shape) % 32 < 16
    return jnp.where(lower, a, roll(b, 16)), jnp.where(lower, roll(a, -16), b)


def sheet_update(water_ref, current_ref, surface_ref, sheet_ref):
    depth = water_ref.shape[0]

    def rows_of(block, carry):
        rows = pl.ds(pl.multiple_of(block * 8, 8), 8)
        surfaces = surface_ref[rows, :]
        water = [water_ref[k, rows, :] for k in range(depth)]
        drag = drag_rate * current_ref[rows, :]
        both = uptake(surfaces)
        inflow_anode = uptake_rate * (both[:, :64] - water[0])
        inflow_cathode = uptake_rate * (roll(both, 64)[:, :64] - water[depth - 1])
        for _ in range(SUBSTEPS):
            below = inflow_anode
            fresh = []
            for k in range(depth):
                if k < depth - 1:
                    mean = base_diffusion + (0.5 * slope_diffusion) * (water[k] + water[k + 1])
                    above = drag * water[k] - mean * (water[k + 1] - water[k])
                else:
                    above = -inflow_cathode
                fresh.append(water[k] + (below - above))
                below = above
            water = fresh
        for k in range(depth):
            sheet_ref[k, rows, :] = water[k]
        return carry

    lax.fori_loop(0, water_ref.shape[1] // 8, rows_of, 0)


def step_kernel(
    pop_hbm,
    mask_ref,
    water_ref,
    current_ref,
    out_ref,
    sheet_ref,
    raw,
    own,
    pack_low,
    pack_high,
    halo_low,
    halo_high,
    fields,
    mask,
    flux,
    psi,
    density,
    force,
    square,
    columns,
    send_pieces,
    recv_pieces,
    load_sem,
    send_sem,
    recv_sem,
    piece_send_sem,
    piece_recv_sem,
):
    side, gx, gy = lax.axis_index("side"), lax.axis_index("gx"), lax.axis_index("gy")
    gx_count, gy_count = lax.axis_size("gx"), lax.axis_size("gy")
    groups = 2 * gy_count
    me = side * gy_count + gy
    x_up = (side, lax.rem(gx + 1, gx_count), gy)
    x_down = (side, lax.rem(gx + gx_count - 1, gx_count), gy)
    y_up = (side, gx, lax.rem(gy + 1, gy_count))
    y_down = (side, gx, lax.rem(gy + gy_count - 1, gy_count))

    def peer(distance):
        other = lax.rem(me + distance, groups)
        return other, (other // gy_count, gx, lax.rem(other, gy_count))

    load = pltpu.make_async_copy(pop_hbm, raw, load_sem)
    load.start()
    barrier = pltpu.get_barrier_semaphore()
    for device in [x_up, x_down] + [peer(d)[1] for d in range(1, groups)]:
        pl.semaphore_signal(barrier, inc=1, device_id=device, device_id_type=MESH)

    copies = []

    def send(src, dst, device):
        slot = len(copies)
        copy = pltpu.make_async_remote_copy(
            src_ref=src,
            dst_ref=dst,
            send_sem=send_sem.at[slot],
            recv_sem=recv_sem.at[slot],
            device_id=device,
            device_id_type=MESH,
        )
        copy.start()
        copies.append(copy)
        return copy

    own[MASK_PLANE, 1:9] = jnp.swapaxes(
        mask_ref[...].astype(jnp.float32).reshape(128, 128), 0, 1
    ).reshape(8, 2, 8, 128)
    square[0:32, 0:64] = water_ref[0]
    square[32:64, 0:64] = water_ref[water_ref.shape[0] - 1]
    columns[...] = jnp.swapaxes(square[...], 0, 1)
    for s in range(2):
        faces = pack_columns(columns.at[pl.ds(0, 64)], 32 * s, 16)
        for g in range(8):
            send_pieces[s * 8 + g, 2:4, :] = faces[2 * g : 2 * g + 2]
    load.wait()
    total = None
    for i in range(LATTICE):
        turned = jnp.swapaxes(raw[i].reshape(128, 128), 0, 1)
        own[i, 1:9] = turned.reshape(8, 2, 8, 128)
    for i in range(LATTICE):
        part = own[i, 1:9].reshape(128, 128)
        total = part if total is None else total + part
    columns[...] = total
    surface = pack_columns(columns, 0, 32)
    for c in range(16):
        send_pieces[c, 0:2, :] = surface[2 * c : 2 * c + 2]
    pl.semaphore_wait(barrier, groups + 1)

    pieces = []
    for d in range(1, groups):
        other, device = peer(d)
        copy = pltpu.make_async_remote_copy(
            src_ref=send_pieces.at[other],
            dst_ref=recv_pieces.at[me],
            send_sem=piece_send_sem.at[d],
            recv_sem=piece_recv_sem.at[d],
            device_id=device,
            device_id_type=MESH,
        )
        copy.start()
        pieces.append(copy)
    main = pl.ds(0, LATTICE + 1)
    y_copies = [
        send(own.at[main, 8], own.at[main, 0], y_up),
        send(own.at[main, 1], own.at[main, 9], y_down),
    ]

    def pack_planes(i, carry):
        low, high = pack_pair(own[i, 1:9, 0], own[i, 1:9, 1])
        pack_low[i, 1:9] = low
        pack_high[i, 1:9] = high
        return carry

    lax.fori_loop(0, LATTICE + 1, pack_planes, 0)
    x_copies = [
        send(pack_low.at[main, pl.ds(1, 8)], halo_high.at[main, pl.ds(1, 8)], x_down),
        send(pack_high.at[main, pl.ds(1, 8)], halo_low.at[main, pl.ds(1, 8)], x_up),
    ]

    recv_pieces[me] = send_pieces[me]
    for copy in pieces:
        copy.wait()
    for c in range(16):
        square[2 * c : 2 * c + 2, :] = recv_pieces[c, 2:4, :]
        square[32 + 2 * c : 34 + 2 * c, :] = recv_pieces[c, 0:2, :]
    own_surface = columns[...]
    unpack_columns(square[0:32, :], columns)
    own_inflow = uptake_rate * (uptake(own_surface) - columns[...])
    own[FLUX_PLANE, 1:9] = own_inflow.reshape(8, 2, 8, 128)
    y_copies += [
        send(own.at[FLUX_PLANE, 8], own.at[FLUX_PLANE, 0], y_up),
        send(own.at[FLUX_PLANE, 1], own.at[FLUX_PLANE, 9], y_down),
    ]
    unpack_columns(square[32:64, :], columns)
    square[...] = jnp.swapaxes(columns[...], 0, 1)
    sheet_update(water_ref, current_ref, square, sheet_ref)

    for copy in y_copies:
        copy.wait()

    def pack_corners(i, carry):
        for t in (0, 9):
            low, high = pack_pair(own[i, t, 0], own[i, t, 1])
            pack_low[i, t] = low
            pack_high[i, t] = high
        return carry

    lax.fori_loop(0, LATTICE + 1, pack_corners, 0)
    low, high = pack_pair(own[FLUX_PLANE, :, 0], own[FLUX_PLANE, :, 1])
    pack_low[FLUX_PLANE] = low
    pack_high[FLUX_PLANE] = high
    for t in (0, 9):
        x_copies += [
            send(pack_low.at[main, t], halo_high.at[main, t], x_down),
            send(pack_high.at[main, t], halo_low.at[main, t], x_up),
        ]
    x_copies += [
        send(pack_low.at[FLUX_PLANE], halo_high.at[FLUX_PLANE], x_down),
        send(pack_high.at[FLUX_PLANE], halo_low.at[FLUX_PLANE], x_up),
    ]
    for copy in x_copies:
        copy.wait()

    lane = lanes_of((8, 128))
    first = lane < 64
    last = lane >= 64
    is_low = lane % 64 < 16
    is_high = lane % 64 >= 48

    def assemble(t, carry):
        start = pl.multiple_of(t * 16 + PAD, 8)
        for i in range(PLANES):
            a, b = own[i, t, 0], own[i, t, 1]
            low, high = halo_low[i, t], halo_high[i, t]

            def join(middle, left, right):
                return jnp.where(is_low, left, jnp.where(is_high, right, middle))

            tiles = (
                (join(roll(a, 16), low, roll(high, 48)), join(roll(b, 16), roll(low, -16), roll(high, 32))),
                (
                    join(roll(a, -16), roll(low, -32), roll(high, 16)),
                    join(roll(b, -16), roll(low, -48), high),
                ),
            )
            for k in range(2):
                if i < LATTICE:
                    shift = velocity_table[i][1]
                    fields[0, i, 0, pl.ds(start + 8 * k - shift, 8), :] = tiles[0][k]
                    fields[0, i, 1, pl.ds(start + 8 * k - shift, 8), :] = tiles[1][k]
                elif i == MASK_PLANE:
                    mask[0, pl.ds(start + 8 * k, 8), :] = tiles[0][k]
                    mask[1, pl.ds(start + 8 * k, 8), :] = tiles[1][k]
                else:
                    flux[pl.ds(start + 8 * k, 8), :] = tiles[0][k]
        return carry

    lax.fori_loop(0, PAIRS, assemble, 0)

    zero = jnp.zeros((8, 128), jnp.float32)

    def layers_sum(a, b):
        return (
            b + jnp.where(last, roll(b, 64), zero),
            a + jnp.where(first, roll(a, 64), zero),
        )

    def layers_difference(a, b):
        return (
            b - jnp.where(last, roll(b, 64), zero),
            jnp.where(first, roll(a, 64), zero) - a,
        )

    def load_fields(now, group, start):
        return [
            fields[now, i, group, pl.ds(start - velocity_table[i][1], 8), :] for i in range(LATTICE)
        ]

    def potentials(now, start):
        for group in range(2):
            loaded = load_fields(now, group, start)
            while len(loaded) > 1:
                loaded = [
                    loaded[k] + loaded[k + 1] if k + 1 < len(loaded) else loaded[k]
                    for k in range(0, len(loaded), 2)
                ]
            rho = loaded[0]
            rows = pl.ds(start, 8)
            density[group, rows, :] = rho
            psi[group, rows, :] = jnp.where(
                mask[group, rows, :] > 0.5, 1.0 - jnp.exp(-rho), wall_potential
            )

    def forces(start):
        centre = [psi[g, pl.ds(start, 8), :] for g in range(2)]
        above = [psi[g, pl.ds(start + 1, 8), :] for g in range(2)]
        below = [psi[g, pl.ds(start - 1, 8), :] for g in range(2)]
        slope = [above[g] - below[g] for g in range(2)]
        base = [(centre[g] + centre[g]) + (above[g] + below[g]) for g in range(2)]
        layers = layers_sum(*centre)
        along_x = [base[g] + layers[g] for g in range(2)]
        slope_layers = layers_sum(*slope)
        along_z = layers_difference(
            *[base[g] + (roll(centre[g], 1) + roll(centre[g], -1)) for g in range(2)]
        )
        scale = 3.0 * KAPPA * relax_time * -coupling / 36.0
        for g in range(2):
            factor = scale * centre[g]
            rows = pl.ds(start, 8)
            force[0, g, rows, :] = factor * (roll(along_x[g], -1) - roll(along_x[g], 1))
            force[1, g, rows, :] = factor * (
                (slope[g] + slope[g]) + slope_layers[g] + (roll(slope[g], 1) + roll(slope[g], -1))
            )
            force[2, g, rows, :] = factor * along_z[g]

    def collide(now, group, start):
        rows = pl.ds(start, 8)
        f = load_fields(now, group, start)
        rho = density[group, rows, :]
        inverse = 1.0 / rho
        odd = [None] + [f[i] - f[i + 1] for i in range(1, LATTICE, 2)]
        moment = (
            odd[1] + odd[4] + odd[5] + (odd[6] + odd[7]),
            odd[2] + odd[4] - odd[5] + (odd[8] + odd[9]),
            odd[3] + odd[6] - odd[7] + (odd[8] - odd[9]),
        )
        flow = [(3.0 * KAPPA) * moment[c] + force[c, group, rows, :] for c in range(3)]
        speed = flow[0] * flow[0] + flow[1] * flow[1] + flow[2] * flow[2]
        scaled = (0.5 / KAPPA) * inverse
        base = KAPPA * rho - (1.5 * KAPPA / (9.0 * KAPPA * KAPPA)) * (speed * inverse)
        double = base + base
        is_pore = mask[group, rows, :] > 0.5
        post = [None] * LATTICE
        post[0] = jnp.where(is_pore, 12.0 * base - (RATE - 1.0) * f[0], f[0])
        for i in range(1, LATTICE, 2):
            velocity = velocity_table[i]
            along = None
            for c in range(3):
                if velocity[c] == 0:
                    continue
                if along is None:
                    along = flow[c]
                elif velocity[c] > 0:
                    along = along + flow[c]
                else:
                    along = along - flow[c]
            if i < 7:
                twice = along + along
                even = double + twice * (along * scaled)
                along = twice
            else:
                even = base + along * (along * scaled)
            up = (even + along) - (RATE - 1.0) * f[i]
            down = (even - along) - (RATE - 1.0) * f[i + 1]
            post[i] = jnp.where(is_pore, up, f[i + 1])
            post[i + 1] = jnp.where(is_pore, down, f[i])
        return post

    def collide_and_move(now, start):
        then = 1 - now
        rows = pl.ds(start, 8)
        a = collide(now, 0, start)
        b = collide(now, 1, start)
        wall_flux = flux[rows, :]
        wall_pair = {1.0 / 18.0: (6.0 / 18.0) * wall_flux, 1.0 / 36.0: (6.0 / 36.0) * wall_flux}
        for i in range(LATTICE):
            shift_x, shift_y, shift_z = velocity_table[i]
            moved = pl.ds(start - shift_y, 8)
            if shift_z == 0:
                fields[then, i, 0, rows, :] = roll(a[i], shift_x)
                fields[then, i, 1, rows, :] = roll(b[i], shift_x)
            elif shift_z == 1:
                fields[then, i, 1, rows, :] = roll(a[i], shift_x)
                wall = a[opposite_index[i]] - wall_pair[weight_table[i]]
                inner = roll(b[i], 64 + shift_x)
                if shift_y == 0:
                    fields[then, i, 0, rows, :] = jnp.where(last, inner, wall)
                else:
                    pltpu.store(fields.at[then, i, 0, rows, :], inner, mask=last)
                    pltpu.store(fields.at[then, i, 0, moved, :], wall, mask=first)
            else:
                fields[then, i, 0, rows, :] = roll(b[i], shift_x)
                wall = b[opposite_index[i]]
                inner = roll(a[i], 64 + shift_x)
                if shift_y == 0:
                    fields[then, i, 1, rows, :] = jnp.where(first, inner, wall)
                else:
                    pltpu.store(fields.at[then, i, 1, rows, :], inner, mask=first)
                    pltpu.store(fields.at[then, i, 1, moved, :], wall, mask=last)

    def one_step(step, carry):
        now = lax.rem(step, 2)
        skip = step // 4
        begin = skip * 8 + PAD
        tiles = 2 * PAIRS - 2 * skip

        def start_of(t):
            return pl.multiple_of(begin + t * 8, 8)

        def potential_pass(t, c):
            for k in range(2):
                potentials(now, start_of(2 * t + k))
            return c

        def force_pass(t, c):
            for k in range(2):
                forces(start_of(2 * t + k))
            return c

        def move_pass(t, c):
            collide_and_move(now, start_of(t))
            return c

        lax.fori_loop(0, tiles // 2, potential_pass, 0)
        lax.fori_loop(0, tiles // 2, force_pass, 0)
        lax.fori_loop(0, tiles, move_pass, 0)
        return carry

    lax.fori_loop(0, STEPS, one_step, 0)

    even_layer = lanes_of((128, 128)) // 32 % 2 == 0
    for i in range(LATTICE):
        rows = pl.ds(PAD + 16 - velocity_table[i][1], 128)
        a, b = fields[STEPS % 2, i, 0, rows, :], fields[STEPS % 2, i, 1, rows, :]
        merged = jnp.where(even_layer, roll(a, -16), roll(b, 16))
        out_ref[i] = jnp.swapaxes(merged, 0, 1).reshape(4, 32, 128)


def on_device(populations, solid_mask, water_sheet, current):
    vmem = pl.BlockSpec(memory_space=pltpu.VMEM)
    lattice, water = pl.pallas_call(
        step_kernel,
        out_shape=(
            jax.ShapeDtypeStruct(populations.shape[1:], jnp.float32),
            jax.ShapeDtypeStruct(water_sheet.shape, jnp.float32),
        ),
        in_specs=[pl.BlockSpec(memory_space=pl.ANY), vmem, vmem, vmem],
        out_specs=(vmem, vmem),
        scratch_shapes=[
            pltpu.VMEM((LATTICE, 4, 32, 128), jnp.float32),
            pltpu.VMEM((PLANES, PAIRS, 2, 8, 128), jnp.float32),
            pltpu.VMEM((PLANES, PAIRS, 8, 128), jnp.float32),
            pltpu.VMEM((PLANES, PAIRS, 8, 128), jnp.float32),
            pltpu.VMEM((PLANES, PAIRS, 8, 128), jnp.float32),
            pltpu.VMEM((PLANES, PAIRS, 8, 128), jnp.float32),
            pltpu.VMEM((2, LATTICE, 2, ROWS, 128), jnp.float32),
            pltpu.VMEM((2, ROWS, 128), jnp.float32),
            pltpu.VMEM((ROWS, 128), jnp.float32),
            pltpu.VMEM((2, ROWS, 128), jnp.float32),
            pltpu.VMEM((2, ROWS, 128), jnp.float32),
            pltpu.VMEM((3, 2, ROWS, 128), jnp.float32),
            pltpu.VMEM((128, 128), jnp.float32),
            pltpu.VMEM((128, 128), jnp.float32),
            pltpu.VMEM((16, 4, 128), jnp.float32),
            pltpu.VMEM((16, 4, 128), jnp.float32),
            pltpu.SemaphoreType.DMA,
            pltpu.SemaphoreType.DMA((12,)),
            pltpu.SemaphoreType.DMA((12,)),
            pltpu.SemaphoreType.DMA((16,)),
            pltpu.SemaphoreType.DMA((16,)),
        ],
        compiler_params=pltpu.CompilerParams(
            collective_id=0, has_side_effects=True, vmem_limit_bytes=48 * 1024 * 1024
        ),
    )(populations[0], solid_mask[0], water_sheet, current)
    return (lattice[None], water)


def solution(mesh):
    in_specs = (
        P("side", None, None, "gx", "gy"),
        P("side", None, "gx", "gy"),
        P(None, "gx", ("side", "gy")),
        P("gx", ("side", "gy")),
    )
    out_specs = (P("side", None, None, "gx", "gy"), P(None, "gx", ("side", "gy")))
    return jax.shard_map(
        on_device, mesh=mesh, in_specs=in_specs, out_specs=out_specs, check_vma=False
    )
```

```python
import functools

import jax
import jax.numpy as jnp
from jax import lax
from jax.experimental import pallas as pl
from jax.experimental.pallas import tpu as pltpu
from jax.sharding import PartitionSpec as P

STEPS = 8
SUBSTEPS = 2
LATTICE = 19
MESH = pl.DeviceIdType.MESH

velocity_table = (
    (0, 0, 0),
    (1, 0, 0),
    (-1, 0, 0),
    (0, 1, 0),
    (0, -1, 0),
    (0, 0, 1),
    (0, 0, -1),
    (1, 1, 0),
    (-1, -1, 0),
    (1, -1, 0),
    (-1, 1, 0),
    (1, 0, 1),
    (-1, 0, -1),
    (1, 0, -1),
    (-1, 0, 1),
    (0, 1, 1),
    (0, -1, -1),
    (0, 1, -1),
    (0, -1, 1),
)
opposite_index = (0, 2, 1, 4, 3, 6, 5, 8, 7, 10, 9, 12, 11, 14, 13, 16, 15, 18, 17)
weight_table = (1.0 / 3.0,) + (1.0 / 18.0,) * 6 + (1.0 / 36.0,) * 12
relax_time = 0.8
coupling = -3.0
wall_potential = 0.4
uptake_rate = 0.02
drag_rate = 0.03
base_diffusion = 0.05
slope_diffusion = 0.015

PAIRS = 10
PAD = 8
ROWS = 16 * PAIRS + 2 * PAD
MASK_PLANE = LATTICE
FLUX_PLANE = LATTICE + 1
PLANES = LATTICE + 2
RATE = 1.0 / relax_time
KAPPA = RATE / 36.0


def roll(values, shift):
    shift = shift % 128
    if shift == 0:
        return values
    return pltpu.roll(values, shift, values.ndim - 1)


def lanes_of(shape):
    return lax.broadcasted_iota(jnp.int32, shape, len(shape) - 1)


def uptake(density_row):
    activity = density_row / (1.0 + density_row)
    return 0.043 + activity * (17.18 + activity * (-39.85 + 36.0 * activity))


def pack_columns(ref, offset, rows):
    lanes = lanes_of((rows, 128))
    packed = None
    for m in range(4):
        part = roll(ref[pl.ds(m, rows, stride=4), :], 32 * m - offset)
        packed = part if packed is None else jnp.where(lanes >= 32 * m, part, packed)
    return packed


def unpack_columns(packed, ref):
    for m in range(4):
        ref[pl.ds(m, packed.shape[0], stride=4), :] = roll(packed, -32 * m)


def pack_pair(a, b):
    lower = lanes_of(a.shape) % 32 < 16
    return jnp.where(lower, a, roll(b, 16)), jnp.where(lower, roll(a, -16), b)


def sheet_update(water_ref, current_ref, surface_ref, sheet_ref):
    depth = water_ref.shape[0]

    def rows_of(block, carry):
        rows = pl.ds(pl.multiple_of(block * 8, 8), 8)
        surfaces = surface_ref[rows, :]
        water = [water_ref[k, rows, :] for k in range(depth)]
        drag = drag_rate * current_ref[rows, :]
        both = uptake(surfaces)
        inflow_anode = uptake_rate * (both[:, :64] - water[0])
        inflow_cathode = uptake_rate * (roll(both, 64)[:, :64] - water[depth - 1])
        for _ in range(SUBSTEPS):
            below = inflow_anode
            fresh = []
            for k in range(depth):
                if k < depth - 1:
                    mean = base_diffusion + (0.5 * slope_diffusion) * (water[k] + water[k + 1])
                    above = drag * water[k] - mean * (water[k + 1] - water[k])
                else:
                    above = -inflow_cathode
                fresh.append(water[k] + (below - above))
                below = above
            water = fresh
        for k in range(depth):
            sheet_ref[k, rows, :] = water[k]
        return carry

    lax.fori_loop(0, water_ref.shape[1] // 8, rows_of, 0)


def step_kernel(
    pop_hbm,
    mask_hbm,
    water_hbm,
    current_hbm,
    out_ref,
    sheet_ref,
    raw,
    raw_mask,
    water_ref,
    current_ref,
    own,
    pack_low,
    pack_high,
    halo_low,
    halo_high,
    fields_even,
    fields_odd,
    coefficients,
    flux,
    slopes,
    centres,
    stage,
    square,
    columns,
    send_pieces,
    recv_pieces,
    load_sem,
    send_sem,
    recv_sem,
    piece_send_sem,
    piece_recv_sem,
):
    side, gx, gy = lax.axis_index("side"), lax.axis_index("gx"), lax.axis_index("gy")
    gx_count, gy_count = lax.axis_size("gx"), lax.axis_size("gy")
    groups = 2 * gy_count
    me = side * gy_count + gy
    x_up = (side, lax.rem(gx + 1, gx_count), gy)
    x_down = (side, lax.rem(gx + gx_count - 1, gx_count), gy)
    y_up = (side, gx, lax.rem(gy + 1, gy_count))
    y_down = (side, gx, lax.rem(gy + gy_count - 1, gy_count))

    def peer(distance):
        other = lax.rem(me + distance, groups)
        return other, (other // gy_count, gx, lax.rem(other, gy_count))

    barrier = pltpu.get_barrier_semaphore()
    for device in [x_up, x_down] + [peer(d)[1] for d in range(1, groups)]:
        pl.semaphore_signal(barrier, inc=1, device_id=device, device_id_type=MESH)
    loads = [
        pltpu.make_async_copy(source, target, load_sem.at[k])
        for k, (source, target) in enumerate(
            ((pop_hbm, raw), (mask_hbm, raw_mask), (water_hbm, water_ref), (current_hbm, current_ref))
        )
    ]
    for load in loads:
        load.start()

    copies = []

    def send(src, dst, device):
        slot = len(copies)
        copy = pltpu.make_async_remote_copy(
            src_ref=src,
            dst_ref=dst,
            send_sem=send_sem.at[slot],
            recv_sem=recv_sem.at[slot],
            device_id=device,
            device_id_type=MESH,
        )
        copy.start()
        copies.append(copy)
        return copy

    loads[0].wait()
    for i in range(LATTICE):
        turned = jnp.swapaxes(raw[i].reshape(128, 128), 0, 1)
        own[i, 1:9] = turned.reshape(8, 2, 8, 128)
    loads[1].wait()
    own[MASK_PLANE, 1:9] = jnp.swapaxes(
        raw_mask[...].astype(jnp.float32).reshape(128, 128), 0, 1
    ).reshape(8, 2, 8, 128)
    loads[2].wait()
    loads[3].wait()
    square[0:32, 0:64] = water_ref[0]
    square[32:64, 0:64] = water_ref[water_ref.shape[0] - 1]
    columns[...] = jnp.swapaxes(square[...], 0, 1)
    for s in range(2):
        faces = pack_columns(columns.at[pl.ds(0, 64)], 32 * s, 16)
        for g in range(8):
            send_pieces[s * 8 + g, 2:4, :] = faces[2 * g : 2 * g + 2]
    total = None
    for i in range(LATTICE):
        part = own[i, 1:9].reshape(128, 128)
        total = part if total is None else total + part
    columns[...] = total
    surface = pack_columns(columns, 0, 32)
    for c in range(16):
        send_pieces[c, 0:2, :] = surface[2 * c : 2 * c + 2]
    main = pl.ds(0, LATTICE + 1)
    inner = pl.ds(1, 8)

    def pack_planes(i):
        low, high = pack_pair(own[i, 1:9, 0], own[i, 1:9, 1])
        pack_low[i, 1:9] = low
        pack_high[i, 1:9] = high

    def pack_four(k, carry):
        for i in range(4):
            pack_planes(4 * k + i)
        return carry

    lax.fori_loop(0, (LATTICE + 1) // 4, pack_four, 0)
    pl.semaphore_wait(barrier, groups + 1)
    pieces = []
    for d in range(1, groups):
        other, device = peer(d)
        copy = pltpu.make_async_remote_copy(
            src_ref=send_pieces.at[other],
            dst_ref=recv_pieces.at[me],
            send_sem=piece_send_sem.at[d],
            recv_sem=piece_recv_sem.at[d],
            device_id=device,
            device_id_type=MESH,
        )
        copy.start()
        pieces.append(copy)

    y_copies = [
        send(own.at[main, 8], own.at[main, 0], y_up),
        send(own.at[main, 1], own.at[main, 9], y_down),
    ]
    x_copies = [
        send(pack_low.at[main, inner], halo_high.at[main, inner], x_down),
        send(pack_high.at[main, inner], halo_low.at[main, inner], x_up),
    ]

    lane = lanes_of((8, 128))
    first = lane < 64
    last = lane >= 64
    is_low = lane % 64 < 16
    is_high = lane % 64 >= 48

    def planes_at(t, planes):
        start = pl.multiple_of(t * 16 + PAD, 8)
        for i in planes:
            for k in range(2):
                rows = pl.ds(start + 8 * k, 8)
                if i < LATTICE:
                    moved = pl.ds(start + 8 * k - velocity_table[i][1], 8)
                    yield i, k, [fields_even.at[0, i, g, moved, :] for g in range(2)]
                elif i == MASK_PLANE:
                    yield i, k, [coefficients.at[0, g, rows, :] for g in range(2)]
                else:
                    yield i, k, [flux.at[rows, :], None]

    def place_own(t, planes):
        for i, k, targets in planes_at(t, planes):
            tile = own[i, t, k]
            for target, shift in zip(targets, (16, -16)):
                if target is not None:
                    target[...] = roll(tile, shift)

    def place_halo(t):
        for i, k, targets in planes_at(t, range(PLANES)):
            low, high = halo_low[i, t], halo_high[i, t]
            for g, target in enumerate(targets):
                if target is not None:
                    pltpu.store(target, roll(low, -16 * k - 32 * g), mask=is_low)
                    pltpu.store(target, roll(high, 48 - 16 * k - 32 * g), mask=is_high)
        start = pl.multiple_of(t * 16 + PAD, 8)
        for k in range(2):
            rows = pl.ds(start + 8 * k, 8)
            for g in range(2):
                pore = coefficients[0, g, rows, :]
                coefficients[1, g, rows, :] = (3.0 * KAPPA) * pore
                coefficients[2, g, rows, :] = (0.5 + 0.5 * (RATE - 1.0)) * pore - 0.5
                coefficients[3, g, rows, :] = 0.5 - (0.5 - 0.5 * (RATE - 1.0)) * pore
                coefficients[4, g, rows, :] = 1.0 - RATE * pore

    def place_inner(t, carry):
        place_own(t, range(LATTICE + 1))
        return carry

    lax.fori_loop(1, 9, place_inner, 0)

    recv_pieces[me] = send_pieces[me]
    for copy in pieces:
        copy.wait()
    for c in range(16):
        square[2 * c : 2 * c + 2, :] = recv_pieces[c, 2:4, :]
        square[32 + 2 * c : 34 + 2 * c, :] = recv_pieces[c, 0:2, :]
    own_surface = columns[...]
    unpack_columns(square[0:32, :], columns)
    own_inflow = uptake_rate * (uptake(own_surface) - columns[...])
    own[FLUX_PLANE, 1:9] = own_inflow.reshape(8, 2, 8, 128)
    y_copies += [
        send(own.at[FLUX_PLANE, 8], own.at[FLUX_PLANE, 0], y_up),
        send(own.at[FLUX_PLANE, 1], own.at[FLUX_PLANE, 9], y_down),
    ]
    pack_planes(FLUX_PLANE)
    x_copies += [
        send(pack_low.at[FLUX_PLANE, inner], halo_high.at[FLUX_PLANE, inner], x_down),
        send(pack_high.at[FLUX_PLANE, inner], halo_low.at[FLUX_PLANE, inner], x_up),
    ]
    unpack_columns(square[32:64, :], columns)
    square[...] = jnp.swapaxes(columns[...], 0, 1)
    sheet_update(water_ref, current_ref, square, sheet_ref)

    for t in range(1, 9):
        place_own(t, [FLUX_PLANE])
    for copy in y_copies:
        copy.wait()

    def pack_corners(k, carry):
        for i in range(3):
            for t in (0, 9):
                low, high = pack_pair(own[3 * k + i, t, 0], own[3 * k + i, t, 1])
                pack_low[3 * k + i, t] = low
                pack_high[3 * k + i, t] = high
        return carry

    lax.fori_loop(0, PLANES // 3, pack_corners, 0)
    corner_copies = []
    for t in (0, 9):
        corner_copies += [
            send(pack_low.at[:, t], halo_high.at[:, t], x_down),
            send(pack_high.at[:, t], halo_low.at[:, t], x_up),
        ]

    for t in (0, 9):
        place_own(t, range(PLANES))

    zero = jnp.zeros((8, 128), jnp.float32)

    def layers_sum(a, b, a_turned, b_turned):
        return b + jnp.where(last, b_turned, zero), a + jnp.where(first, a_turned, zero)

    def layers_difference(a, b, a_turned, b_turned):
        return b - jnp.where(last, b_turned, zero), jnp.where(first, a_turned, zero) - a

    def load_fields(fields, group, start):
        return [
            fields[i, group, pl.ds(start - velocity_table[i][1], 8), :] for i in range(LATTICE)
        ]

    def potentials(fields, slopes, start):
        rows = pl.ds(start, 8)
        potential = []
        for g in range(2):
            loaded = load_fields(fields, g, start)
            while len(loaded) > 1:
                loaded = [
                    loaded[k] + loaded[k + 1] if k + 1 < len(loaded) else loaded[k]
                    for k in range(0, len(loaded), 2)
                ]
            rho = loaded[0]
            pore = coefficients[0, g, rows, :]
            is_pore = pore > 0.5
            value = jnp.where(is_pore, 1.0 - jnp.exp(-rho), wall_potential)
            potential.append(value)
            centres[0, g, rows, :] = (KAPPA * pore) * rho
            centres[1, g, rows, :] = (0.5 / KAPPA) / rho
            centres[2, g, rows, :] = (3.0 * KAPPA * relax_time * -coupling / 36.0) * (pore * value)
        right = [roll(p, -1) for p in potential]
        left = [roll(p, 1) for p in potential]
        turned = [roll(p, 64) for p in potential]
        right_turned = [roll(p, 63) for p in potential]
        left_turned = [roll(p, 65) for p in potential]
        slope_x = [right[g] - left[g] for g in range(2)]
        slope_x_turned = [right_turned[g] - left_turned[g] for g in range(2)]
        wide = [(potential[g] + potential[g]) + (right[g] + left[g]) for g in range(2)]
        wide_turned = [(turned[g] + turned[g]) + (right_turned[g] + left_turned[g]) for g in range(2)]
        layers = layers_sum(*potential, *turned)
        slope_z = layers_difference(*potential, *turned)
        slope_x_layers = layers_sum(*slope_x, *slope_x_turned)
        slope_z_wide = layers_difference(*wide, *wide_turned)
        for g in range(2):
            slopes[0, g, rows, :] = slope_x[g]
            slopes[1, g, rows, :] = wide[g] + layers[g]
            slopes[2, g, rows, :] = slope_z[g]
            centres[3, g, rows, :] = (slope_x[g] + slope_x[g]) + slope_x_layers[g]
            centres[4, g, rows, :] = slope_z_wide[g]

    def collide(fields, slopes, g, start):
        rows = pl.ds(start, 8)
        above, below = pl.ds(start + 1, 8), pl.ds(start - 1, 8)
        f = load_fields(fields, g, start)
        odd = [None] + [f[i] - f[i + 1] for i in range(1, LATTICE, 2)]
        sums = [None] + [f[i] + f[i + 1] for i in range(1, LATTICE, 2)]
        moment = (
            (odd[1] + odd[4]) + (odd[5] + (odd[6] + odd[7])),
            (odd[2] + odd[4]) + ((odd[8] + odd[9]) - odd[5]),
            (odd[3] + odd[6]) + ((odd[8] - odd[9]) - odd[7]),
        )
        gradient = (
            centres[3, g, rows, :] + (slopes[0, g, above, :] + slopes[0, g, below, :]),
            slopes[1, g, above, :] - slopes[1, g, below, :],
            centres[4, g, rows, :] + (slopes[2, g, above, :] + slopes[2, g, below, :]),
        )
        factor = centres[2, g, rows, :]
        three = coefficients[1, g, rows, :]
        even_part = coefficients[2, g, rows, :]
        odd_part = coefficients[3, g, rows, :]
        flow = [three * moment[c] + factor * gradient[c] for c in range(3)]
        speed = flow[0] * flow[0] + flow[1] * flow[1] + flow[2] * flow[2]
        scaled = centres[1, g, rows, :]
        base = centres[0, g, rows, :] - (1.0 / 3.0) * (speed * scaled)
        double = base + base
        post = [None] * LATTICE
        post[0] = 12.0 * base + coefficients[4, g, rows, :] * f[0]
        for p in range(1, 10):
            i = 2 * p - 1
            velocity = velocity_table[i]
            along = None
            for c in range(3):
                if velocity[c] == 0:
                    continue
                if along is None:
                    along = flow[c]
                elif velocity[c] > 0:
                    along = along + flow[c]
                else:
                    along = along - flow[c]
            if i < 7:
                twice = along + along
                even = double + twice * (along * scaled)
                along = twice
            else:
                even = base + along * (along * scaled)
            even = even - even_part * sums[p]
            along = along - odd_part * odd[p]
            post[i] = even + along
            post[i + 1] = even - along
        return post

    def relax(fields, slopes, start, half):
        a = collide(fields, slopes, 0, start)
        b = collide(fields, slopes, 1, start)
        wall_flux = flux[pl.ds(start, 8), :]
        walls = 0
        for i in range(LATTICE):
            stage[half, i] = a[i]
            stage[half, LATTICE + i] = b[i]
            if velocity_table[i][2] == 1:
                stage[half, 2 * LATTICE + walls] = (
                    a[opposite_index[i]] - (6.0 * weight_table[i]) * wall_flux
                )
                walls += 1

    def move(fields, start, half):
        rows = pl.ds(start, 8)
        walls = 0
        for i in range(LATTICE):
            shift_x, shift_y, shift_z = velocity_table[i]
            moved = pl.ds(start - shift_y, 8)
            a, b = stage[half, i], stage[half, LATTICE + i]
            if shift_z == 0:
                fields[i, 0, rows, :] = roll(a, shift_x)
                fields[i, 1, rows, :] = roll(b, shift_x)
            elif shift_z == 1:
                fields[i, 1, rows, :] = roll(a, shift_x)
                pltpu.store(fields.at[i, 0, rows, :], roll(b, 64 + shift_x), mask=last)
                wall = stage[half, 2 * LATTICE + walls]
                pltpu.store(fields.at[i, 0, moved, :], wall, mask=first)
                walls += 1
            else:
                fields[i, 0, rows, :] = roll(b, shift_x)
                pltpu.store(fields.at[i, 1, rows, :], roll(a, 64 + shift_x), mask=first)
                wall = stage[half, LATTICE + opposite_index[i]]
                pltpu.store(fields.at[i, 1, moved, :], wall, mask=last)

    def run_steps(tiles, begin, end):
        starts = [tile * 8 + PAD for tile in tiles]

        def one_step(step, now, then):
            for start in starts:
                potentials(now, slopes.at[step], start)
            for slot, start in enumerate(starts):
                relax(now, slopes.at[step], start, slot)
                if slot % 2 == 1 and slot > 2:
                    for done in (slot - 3, slot - 2):
                        move(then, starts[done], done)
            for done in (len(starts) - 2, len(starts) - 1):
                move(then, starts[done], done)

        def two_steps(half, carry):
            one_step(2 * half, fields_even.at[half], fields_odd.at[half])
            one_step(2 * half + 1, fields_odd.at[half], fields_even.at[half + 1])
            return carry

        lax.fori_loop(begin // 2, end // 2, two_steps, 0)

    for copy in x_copies:
        copy.wait()

    def halo_inner(t, carry):
        place_halo(t)
        return carry

    lax.fori_loop(1, 9, halo_inner, 0)
    run_steps(range(2, 18), 0, STEPS)
    for copy in corner_copies:
        copy.wait()
    for t in (0, 9):
        place_halo(t)
    for base in range(2):
        ends = [base + k for k in range(3)] + [17 - base + k for k in range(3)]
        run_steps(ends, base * STEPS // 2, (base + 1) * STEPS // 2)

    even_layer = lanes_of((128, 128)) // 32 % 2 == 0
    for i in range(LATTICE):
        rows = pl.ds(PAD + 16 - velocity_table[i][1], 128)
        a, b = fields_even[STEPS // 2, i, 0, rows, :], fields_even[STEPS // 2, i, 1, rows, :]
        merged = jnp.where(even_layer, roll(a, -16), roll(b, 16))
        out_ref[i] = jnp.swapaxes(merged, 0, 1).reshape(4, 32, 128)


def on_device(populations, solid_mask, water_sheet, current):
    arguments = (populations[0], solid_mask[0], water_sheet, current)
    vmem = pl.BlockSpec(memory_space=pltpu.VMEM)
    hbm = pl.BlockSpec(memory_space=pltpu.HBM)
    lattice, water = pl.pallas_call(
        step_kernel,
        out_shape=(
            jax.ShapeDtypeStruct(populations.shape[1:], jnp.float32),
            jax.ShapeDtypeStruct(water_sheet.shape, jnp.float32),
        ),
        in_specs=[hbm, hbm, hbm, hbm],
        out_specs=(vmem, vmem),
        scratch_shapes=[
            pltpu.VMEM((LATTICE, 4, 32, 128), jnp.float32),
            pltpu.VMEM(solid_mask.shape[1:], jnp.int32),
            pltpu.VMEM(water_sheet.shape, jnp.float32),
            pltpu.VMEM(current.shape, jnp.float32),
            pltpu.VMEM((PLANES, PAIRS, 2, 8, 128), jnp.float32),
            pltpu.VMEM((PLANES, PAIRS, 8, 128), jnp.float32),
            pltpu.VMEM((PLANES, PAIRS, 8, 128), jnp.float32),
            pltpu.VMEM((PLANES, PAIRS, 8, 128), jnp.float32),
            pltpu.VMEM((PLANES, PAIRS, 8, 128), jnp.float32),
            pltpu.VMEM((STEPS // 2 + 1, LATTICE, 2, ROWS, 128), jnp.float32),
            pltpu.VMEM((STEPS // 2, LATTICE, 2, ROWS, 128), jnp.float32),
            pltpu.VMEM((5, 2, ROWS, 128), jnp.float32),
            pltpu.VMEM((ROWS, 128), jnp.float32),
            pltpu.VMEM((STEPS, 3, 2, ROWS, 128), jnp.float32),
            pltpu.VMEM((5, 2, ROWS, 128), jnp.float32),
            pltpu.VMEM((16, 2 * LATTICE + 5, 8, 128), jnp.float32),
            pltpu.VMEM((128, 128), jnp.float32),
            pltpu.VMEM((128, 128), jnp.float32),
            pltpu.VMEM((16, 4, 128), jnp.float32),
            pltpu.VMEM((16, 4, 128), jnp.float32),
            pltpu.SemaphoreType.DMA((4,)),
            pltpu.SemaphoreType.DMA((12,)),
            pltpu.SemaphoreType.DMA((12,)),
            pltpu.SemaphoreType.DMA((16,)),
            pltpu.SemaphoreType.DMA((16,)),
        ],
        compiler_params=pltpu.CompilerParams(
            collective_id=0, has_side_effects=True, vmem_limit_bytes=50 * 1024 * 1024
        ),
    )(*[pltpu.with_memory_space_constraint(value, pltpu.HBM) for value in arguments])
    return (lattice[None], water)


def solution(mesh):
    in_specs = (
        P("side", None, None, "gx", "gy"),
        P("side", None, "gx", "gy"),
        P(None, "gx", ("side", "gy")),
        P("gx", ("side", "gy")),
    )
    out_specs = (P("side", None, None, "gx", "gy"), P(None, "gx", ("side", "gy")))
    return jax.shard_map(
        on_device, mesh=mesh, in_specs=in_specs, out_specs=out_specs, check_vma=False
    )
```

```python
import functools

import jax
import jax.numpy as jnp
from jax import lax
from jax.experimental import pallas as pl
from jax.experimental.pallas import tpu as pltpu
from jax.sharding import PartitionSpec as P

STEPS = 8
SUBSTEPS = 2
LATTICE = 19
MESH = pl.DeviceIdType.MESH

velocity_table = (
    (0, 0, 0),
    (1, 0, 0),
    (-1, 0, 0),
    (0, 1, 0),
    (0, -1, 0),
    (0, 0, 1),
    (0, 0, -1),
    (1, 1, 0),
    (-1, -1, 0),
    (1, -1, 0),
    (-1, 1, 0),
    (1, 0, 1),
    (-1, 0, -1),
    (1, 0, -1),
    (-1, 0, 1),
    (0, 1, 1),
    (0, -1, -1),
    (0, 1, -1),
    (0, -1, 1),
)
opposite_index = (0, 2, 1, 4, 3, 6, 5, 8, 7, 10, 9, 12, 11, 14, 13, 16, 15, 18, 17)
weight_table = (1.0 / 3.0,) + (1.0 / 18.0,) * 6 + (1.0 / 36.0,) * 12
relax_time = 0.8
coupling = -3.0
wall_potential = 0.4
uptake_rate = 0.02
drag_rate = 0.03
base_diffusion = 0.05
slope_diffusion = 0.015

PAIRS = 10
PAD = 8
ROWS = 16 * PAIRS + 2 * PAD
MASK_PLANE = LATTICE
FLUX_PLANE = LATTICE + 1
PLANES = LATTICE + 2
RATE = 1.0 / relax_time
KAPPA = RATE / 36.0


def roll(values, shift):
    shift = shift % 128
    if shift == 0:
        return values
    return pltpu.roll(values, shift, values.ndim - 1)


def lanes_of(shape):
    return lax.broadcasted_iota(jnp.int32, shape, len(shape) - 1)


def uptake(density_row):
    activity = density_row / (1.0 + density_row)
    return 0.043 + activity * (17.18 + activity * (-39.85 + 36.0 * activity))


def pack_columns(ref, offset, rows):
    lanes = lanes_of((rows, 128))
    packed = None
    for m in range(4):
        part = roll(ref[pl.ds(m, rows, stride=4), :], 32 * m - offset)
        packed = part if packed is None else jnp.where(lanes >= 32 * m, part, packed)
    return packed


def unpack_columns(packed, ref):
    for m in range(4):
        ref[pl.ds(m, packed.shape[0], stride=4), :] = roll(packed, -32 * m)


def pack_pair(a, b):
    lower = lanes_of(a.shape) % 32 < 16
    return jnp.where(lower, a, roll(b, 16)), jnp.where(lower, roll(a, -16), b)


def sheet_update(water_ref, current_ref, surface_ref, sheet_ref):
    depth = water_ref.shape[0]

    def rows_of(block, carry):
        rows = pl.ds(pl.multiple_of(block * 8, 8), 8)
        surfaces = surface_ref[rows, :]
        water = [water_ref[k, rows, :] for k in range(depth)]
        drag = drag_rate * current_ref[rows, :]
        both = uptake(surfaces)
        inflow_anode = uptake_rate * (both[:, :64] - water[0])
        inflow_cathode = uptake_rate * (roll(both, 64)[:, :64] - water[depth - 1])
        for _ in range(SUBSTEPS):
            below = inflow_anode
            fresh = []
            for k in range(depth):
                if k < depth - 1:
                    mean = base_diffusion + (0.5 * slope_diffusion) * (water[k] + water[k + 1])
                    above = drag * water[k] - mean * (water[k + 1] - water[k])
                else:
                    above = -inflow_cathode
                fresh.append(water[k] + (below - above))
                below = above
            water = fresh
        for k in range(depth):
            sheet_ref[k, rows, :] = water[k]
        return carry

    lax.fori_loop(0, water_ref.shape[1] // 8, rows_of, 0)


def step_kernel(
    pop_hbm,
    mask_hbm,
    water_hbm,
    current_hbm,
    out_ref,
    sheet_ref,
    window,
    flux_window,
    raw_mask,
    water_ref,
    current_ref,
    own,
    pack_low,
    pack_high,
    halo_low,
    halo_high,
    fields_even,
    fields_odd,
    coefficients,
    flux,
    slopes,
    centres,
    stage,
    square,
    columns,
    send_pieces,
    recv_pieces,
    load_sem,
    send_sem,
    recv_sem,
    piece_send_sem,
    piece_recv_sem,
):
    side, gx, gy = lax.axis_index("side"), lax.axis_index("gx"), lax.axis_index("gy")
    gx_count, gy_count = lax.axis_size("gx"), lax.axis_size("gy")
    groups = 2 * gy_count
    me = side * gy_count + gy
    x_up = (side, lax.rem(gx + 1, gx_count), gy)
    x_down = (side, lax.rem(gx + gx_count - 1, gx_count), gy)
    y_up = (side, gx, lax.rem(gy + 1, gy_count))
    y_down = (side, gx, lax.rem(gy + gy_count - 1, gy_count))

    def peer(distance):
        other = lax.rem(me + distance, groups)
        return other, (other // gy_count, gx, lax.rem(other, gy_count))

    barrier = pltpu.get_barrier_semaphore()
    for device in [x_up, x_down] + [peer(d)[1] for d in range(1, groups)]:
        pl.semaphore_signal(barrier, inc=1, device_id=device, device_id_type=MESH)
    loads = [
        pltpu.make_async_copy(source, target, load_sem.at[k])
        for k, (source, target) in enumerate(
            ((pop_hbm, window.at[pl.ds(0, LATTICE), :, :, pl.ds(16, 32), :]), (mask_hbm, raw_mask), (water_hbm, water_ref), (current_hbm, current_ref))
        )
    ]
    for load in loads:
        load.start()

    copies = []

    def prepare(src, dst, device):
        slot = len(copies)
        copy = pltpu.make_async_remote_copy(
            src_ref=src,
            dst_ref=dst,
            send_sem=send_sem.at[slot],
            recv_sem=recv_sem.at[slot],
            device_id=device,
            device_id_type=MESH,
        )
        copies.append(copy)
        return copy

    def send(src, dst, device):
        copy = prepare(src, dst, device)
        copy.start()
        return copy

    loads[0].wait()
    pl.semaphore_wait(barrier, groups + 1)

    lattice = pl.ds(0, LATTICE)
    edges = ((16, 48, x_down), (32, 0, x_up))
    x_copies = [
        send(
            window.at[lattice, :, :, pl.ds(source, 16), :], window.at[lattice, :, :, pl.ds(target, 16), :], device
        )
        for source, target, device in edges
    ]
    loads[1].wait()
    window[MASK_PLANE, :, :, 16:48, :] = raw_mask[...].astype(jnp.float32)
    x_copies += [
        send(
            window.at[MASK_PLANE, :, :, pl.ds(source, 16), :],
            window.at[MASK_PLANE, :, :, pl.ds(target, 16), :],
            device,
        )
        for source, target, device in edges
    ]

    loads[2].wait()
    loads[3].wait()
    square[0:32, 0:64] = water_ref[0]
    square[32:64, 0:64] = water_ref[water_ref.shape[0] - 1]
    columns[...] = jnp.swapaxes(square[...], 0, 1)
    for s in range(2):
        faces = pack_columns(columns.at[pl.ds(0, 64)], 32 * s, 16)
        for g in range(8):
            send_pieces[s * 8 + g, 2:4, :] = faces[2 * g : 2 * g + 2]
    total = None
    for i in range(LATTICE):
        part = window[i, 0, 0, 16:48, :]
        total = part if total is None else total + part
    square[0:32, :] = total
    columns[...] = jnp.swapaxes(square[...], 0, 1)
    surface = pack_columns(columns, 0, 32)
    for c in range(16):
        send_pieces[c, 0:2, :] = surface[2 * c : 2 * c + 2]
    pieces = []
    for d in range(1, groups):
        other, device = peer(d)
        copy = pltpu.make_async_remote_copy(
            src_ref=send_pieces.at[other],
            dst_ref=recv_pieces.at[me],
            send_sem=piece_send_sem.at[d],
            recv_sem=piece_recv_sem.at[d],
            device_id=device,
            device_id_type=MESH,
        )
        copy.start()
        pieces.append(copy)

    for i in range(LATTICE + 1):
        turned = jnp.swapaxes(window[i, :, :, 16:48, :].reshape(128, 128), 0, 1)
        own[i, 1] = turned[0:16].reshape(2, 8, 128)
        own[i, 8] = turned[112:128].reshape(2, 8, 128)
    main = pl.ds(0, LATTICE + 1)
    y_copies = [
        send(own.at[main, 8], own.at[main, 0], y_up),
        send(own.at[main, 1], own.at[main, 9], y_down),
    ]

    lane = lanes_of((8, 128))
    first = lane < 64
    last = lane >= 64
    is_low = lane % 64 < 16
    is_high = lane % 64 >= 48

    def planes_at(t, planes):
        start = pl.multiple_of(t * 16 + PAD, 8)
        for i in planes:
            for k in range(2):
                rows = pl.ds(start + 8 * k, 8)
                if i < LATTICE:
                    moved = pl.ds(start + 8 * k - velocity_table[i][1], 8)
                    yield i, k, [fields_even.at[0, i, g, moved, :] for g in range(2)]
                elif i == MASK_PLANE:
                    yield i, k, [coefficients.at[0, g, rows, :] for g in range(2)]
                else:
                    yield i, k, [flux.at[rows, :], None]

    def set_coefficients(g, rows, pore):
        coefficients[0, g, rows, :] = pore
        coefficients[1, g, rows, :] = (3.0 * KAPPA) * pore
        coefficients[2, g, rows, :] = (0.5 + 0.5 * (RATE - 1.0)) * pore - 0.5
        coefficients[3, g, rows, :] = 0.5 - (0.5 - 0.5 * (RATE - 1.0)) * pore
        coefficients[4, g, rows, :] = 1.0 - RATE * pore

    def place_own(t, planes):
        for i, k, targets in planes_at(t, planes):
            tile = own[i, t, k]
            for target, shift in zip(targets, (16, -16)):
                if target is not None:
                    target[...] = roll(tile, shift)

    def place_halo(t, planes):
        for i, k, targets in planes_at(t, planes):
            low, high = halo_low[i, t // 9], halo_high[i, t // 9]
            for g, target in enumerate(targets):
                if target is not None:
                    pltpu.store(target, roll(low, -16 * k - 32 * g), mask=is_low)
                    pltpu.store(target, roll(high, 48 - 16 * k - 32 * g), mask=is_high)
        start = pl.multiple_of(t * 16 + PAD, 8)
        for k in range(2):
            rows = pl.ds(start + 8 * k, 8)
            for g in range(2):
                set_coefficients(g, rows, coefficients[0, g, rows, :])

    recv_pieces[me] = send_pieces[me]
    for copy in pieces:
        copy.wait()
    for c in range(16):
        square[2 * c : 2 * c + 2, :] = recv_pieces[c, 2:4, :]
        square[32 + 2 * c : 34 + 2 * c, :] = recv_pieces[c, 0:2, :]
    own_surface = columns[...]
    unpack_columns(square[0:32, :], columns)
    own_inflow = uptake_rate * (uptake(own_surface) - columns[...])
    own[FLUX_PLANE, 1] = own_inflow[0:16].reshape(2, 8, 128)
    own[FLUX_PLANE, 8] = own_inflow[112:128].reshape(2, 8, 128)
    flux_window[16:48, :] = jnp.swapaxes(own_inflow, 0, 1)[0:32]
    y_copies += [
        send(own.at[FLUX_PLANE, 8], own.at[FLUX_PLANE, 0], y_up),
        send(own.at[FLUX_PLANE, 1], own.at[FLUX_PLANE, 9], y_down),
    ]
    x_copies += [
        send(flux_window.at[pl.ds(source, 16), :], flux_window.at[pl.ds(target, 16), :], device)
        for source, target, device in edges
    ]
    unpack_columns(square[32:64, :], columns)
    square[...] = jnp.swapaxes(columns[...], 0, 1)
    sheet_update(water_ref, current_ref, square, sheet_ref)

    corner_copies = []
    for end in range(2):
        corner_copies += [
            prepare(pack_low.at[:, end], halo_high.at[:, end], x_down),
            prepare(pack_high.at[:, end], halo_low.at[:, end], x_up),
        ]

    def pack_corners(k, carry):
        for i in range(3):
            for t in (0, 9):
                low, high = pack_pair(own[3 * k + i, t, 0], own[3 * k + i, t, 1])
                pack_low[3 * k + i, t // 9] = low
                pack_high[3 * k + i, t // 9] = high
        return carry

    def pass_corners():
        for copy in y_copies:
            copy.wait()
        lax.fori_loop(0, PLANES // 3, pack_corners, 0)
        for copy in corner_copies:
            copy.start()
        for t in (0, 9):
            place_own(t, range(PLANES))

    zero = jnp.zeros((8, 128), jnp.float32)

    def layers_sum(a, b, a_turned, b_turned):
        return b + jnp.where(last, b_turned, zero), a + jnp.where(first, a_turned, zero)

    def layers_difference(a, b, a_turned, b_turned):
        return b - jnp.where(last, b_turned, zero), jnp.where(first, a_turned, zero) - a

    def load_fields(fields, group, start):
        return [
            fields[i, group, pl.ds(start - velocity_table[i][1], 8), :] for i in range(LATTICE)
        ]

    def potentials(fields, slopes, start):
        rows = pl.ds(start, 8)
        potential = []
        for g in range(2):
            loaded = load_fields(fields, g, start)
            while len(loaded) > 1:
                loaded = [
                    loaded[k] + loaded[k + 1] if k + 1 < len(loaded) else loaded[k]
                    for k in range(0, len(loaded), 2)
                ]
            rho = loaded[0]
            pore = coefficients[0, g, rows, :]
            is_pore = pore > 0.5
            value = jnp.where(is_pore, 1.0 - jnp.exp(-rho), wall_potential)
            potential.append(value)
            centres[0, g, rows, :] = (KAPPA * pore) * rho
            centres[1, g, rows, :] = (0.5 / KAPPA) / rho
            centres[2, g, rows, :] = (3.0 * KAPPA * relax_time * -coupling / 36.0) * (pore * value)
        right = [roll(p, -1) for p in potential]
        left = [roll(p, 1) for p in potential]
        turned = [roll(p, 64) for p in potential]
        right_turned = [roll(p, 63) for p in potential]
        left_turned = [roll(p, 65) for p in potential]
        slope_x = [right[g] - left[g] for g in range(2)]
        slope_x_turned = [right_turned[g] - left_turned[g] for g in range(2)]
        wide = [(potential[g] + potential[g]) + (right[g] + left[g]) for g in range(2)]
        wide_turned = [(turned[g] + turned[g]) + (right_turned[g] + left_turned[g]) for g in range(2)]
        layers = layers_sum(*potential, *turned)
        slope_z = layers_difference(*potential, *turned)
        slope_x_layers = layers_sum(*slope_x, *slope_x_turned)
        slope_z_wide = layers_difference(*wide, *wide_turned)
        for g in range(2):
            slopes[0, g, rows, :] = slope_x[g]
            slopes[1, g, rows, :] = wide[g] + layers[g]
            slopes[2, g, rows, :] = slope_z[g]
            centres[3, g, rows, :] = (slope_x[g] + slope_x[g]) + slope_x_layers[g]
            centres[4, g, rows, :] = slope_z_wide[g]

    def collide(fields, slopes, g, start):
        rows = pl.ds(start, 8)
        above, below = pl.ds(start + 1, 8), pl.ds(start - 1, 8)
        f = load_fields(fields, g, start)
        odd = [None] + [f[i] - f[i + 1] for i in range(1, LATTICE, 2)]
        sums = [None] + [f[i] + f[i + 1] for i in range(1, LATTICE, 2)]
        moment = (
            (odd[1] + odd[4]) + (odd[5] + (odd[6] + odd[7])),
            (odd[2] + odd[4]) + ((odd[8] + odd[9]) - odd[5]),
            (odd[3] + odd[6]) + ((odd[8] - odd[9]) - odd[7]),
        )
        gradient = (
            centres[3, g, rows, :] + (slopes[0, g, above, :] + slopes[0, g, below, :]),
            slopes[1, g, above, :] - slopes[1, g, below, :],
            centres[4, g, rows, :] + (slopes[2, g, above, :] + slopes[2, g, below, :]),
        )
        factor = centres[2, g, rows, :]
        three = coefficients[1, g, rows, :]
        even_part = coefficients[2, g, rows, :]
        odd_part = coefficients[3, g, rows, :]
        flow = [three * moment[c] + factor * gradient[c] for c in range(3)]
        speed = flow[0] * flow[0] + flow[1] * flow[1] + flow[2] * flow[2]
        scaled = centres[1, g, rows, :]
        base = centres[0, g, rows, :] - (1.0 / 3.0) * (speed * scaled)
        double = base + base
        post = [None] * LATTICE
        post[0] = 12.0 * base + coefficients[4, g, rows, :] * f[0]
        for p in range(1, 10):
            i = 2 * p - 1
            velocity = velocity_table[i]
            along = None
            for c in range(3):
                if velocity[c] == 0:
                    continue
                if along is None:
                    along = flow[c]
                elif velocity[c] > 0:
                    along = along + flow[c]
                else:
                    along = along - flow[c]
            if i < 7:
                twice = along + along
                even = double + twice * (along * scaled)
                along = twice
            else:
                even = base + along * (along * scaled)
            even = even - even_part * sums[p]
            along = along - odd_part * odd[p]
            post[i] = even + along
            post[i + 1] = even - along
        return post

    def relax(fields, slopes, start, half):
        a = collide(fields, slopes, 0, start)
        b = collide(fields, slopes, 1, start)
        wall_flux = flux[pl.ds(start, 8), :]
        walls = 0
        for i in range(LATTICE):
            stage[half, i] = a[i]
            stage[half, LATTICE + i] = b[i]
            if velocity_table[i][2] == 1:
                stage[half, 2 * LATTICE + walls] = (
                    a[opposite_index[i]] - (6.0 * weight_table[i]) * wall_flux
                )
                walls += 1

    def move(fields, start, half):
        rows = pl.ds(start, 8)
        walls = 0
        for i in range(LATTICE):
            shift_x, shift_y, shift_z = velocity_table[i]
            moved = pl.ds(start - shift_y, 8)
            a, b = stage[half, i], stage[half, LATTICE + i]
            if shift_z == 0:
                fields[i, 0, rows, :] = roll(a, shift_x)
                fields[i, 1, rows, :] = roll(b, shift_x)
            elif shift_z == 1:
                fields[i, 1, rows, :] = roll(a, shift_x)
                pltpu.store(fields.at[i, 0, rows, :], roll(b, 64 + shift_x), mask=last)
                wall = stage[half, 2 * LATTICE + walls]
                pltpu.store(fields.at[i, 0, moved, :], wall, mask=first)
                walls += 1
            else:
                fields[i, 0, rows, :] = roll(b, shift_x)
                pltpu.store(fields.at[i, 1, rows, :], roll(a, 64 + shift_x), mask=first)
                wall = stage[half, LATTICE + opposite_index[i]]
                pltpu.store(fields.at[i, 1, moved, :], wall, mask=last)

    def run_steps(tiles, begin, end):
        starts = [tile * 8 + PAD for tile in tiles]

        def one_step(step, now, then):
            for start in starts:
                potentials(now, slopes.at[step], start)
            for slot, start in enumerate(starts):
                relax(now, slopes.at[step], start, slot)
                if slot % 2 == 1 and slot > 2:
                    for done in (slot - 3, slot - 2):
                        move(then, starts[done], done)
            for done in (len(starts) - 2, len(starts) - 1):
                move(then, starts[done], done)

        def two_steps(half, carry):
            one_step(2 * half, fields_even.at[half], fields_odd.at[half])
            one_step(2 * half + 1, fields_odd.at[half], fields_even.at[half + 1])
            return carry

        lax.fori_loop(begin // 2, end // 2, two_steps, 0)

    for copy in x_copies[:4]:
        copy.wait()
    for i in range(LATTICE + 1):
        for g in range(2):
            turned = jnp.swapaxes(window[i, :, g].reshape(128, 128), 0, 1)
            if i < LATTICE:
                fields_even[0, i, g, pl.ds(PAD + 16 - velocity_table[i][1], 128), :] = turned
            else:
                set_coefficients(g, pl.ds(PAD + 16, 128), turned)
    for copy in x_copies[4:]:
        copy.wait()
    flux[pl.ds(PAD + 16, 128), :] = jnp.swapaxes(flux_window[...], 0, 1)
    pass_corners()
    run_steps(range(2, 18), 0, STEPS)
    for copy in corner_copies:
        copy.wait()
    for t in (0, 9):
        place_halo(t, range(PLANES))
    for base in range(2):
        ends = [base + k for k in range(3)] + [17 - base + k for k in range(3)]
        run_steps(ends, base * STEPS // 2, (base + 1) * STEPS // 2)

    for i in range(LATTICE):
        rows = pl.ds(PAD + 16 - velocity_table[i][1], 128)
        for g in range(2):
            turned = jnp.swapaxes(fields_even[STEPS // 2, i, g, rows, :], 0, 1)
            out_ref[i, g] = turned[16:48]
            out_ref[i, g + 2] = turned[80:112]


def on_device(populations, solid_mask, water_sheet, current):
    arguments = (
        populations.reshape(LATTICE, 2, 2, 32, 128),
        solid_mask.reshape(2, 2, 32, 128),
        water_sheet,
        current,
    )
    vmem = pl.BlockSpec(memory_space=pltpu.VMEM)
    hbm = pl.BlockSpec(memory_space=pltpu.HBM)
    lattice, water = pl.pallas_call(
        step_kernel,
        out_shape=(
            jax.ShapeDtypeStruct(populations.shape[1:], jnp.float32),
            jax.ShapeDtypeStruct(water_sheet.shape, jnp.float32),
        ),
        in_specs=[hbm, hbm, hbm, hbm],
        out_specs=(vmem, vmem),
        scratch_shapes=[
            pltpu.VMEM((LATTICE + 1, 2, 2, 64, 128), jnp.float32),
            pltpu.VMEM((128, 128), jnp.float32),
            pltpu.VMEM((2, 2, 32, 128), jnp.int32),
            pltpu.VMEM(water_sheet.shape, jnp.float32),
            pltpu.VMEM(current.shape, jnp.float32),
            pltpu.VMEM((PLANES, PAIRS, 2, 8, 128), jnp.float32),
            pltpu.VMEM((PLANES, 2, 8, 128), jnp.float32),
            pltpu.VMEM((PLANES, 2, 8, 128), jnp.float32),
            pltpu.VMEM((PLANES, 2, 8, 128), jnp.float32),
            pltpu.VMEM((PLANES, 2, 8, 128), jnp.float32),
            pltpu.VMEM((STEPS // 2 + 1, LATTICE, 2, ROWS, 128), jnp.float32),
            pltpu.VMEM((STEPS // 2, LATTICE, 2, ROWS, 128), jnp.float32),
            pltpu.VMEM((5, 2, ROWS, 128), jnp.float32),
            pltpu.VMEM((ROWS, 128), jnp.float32),
            pltpu.VMEM((STEPS, 3, 2, ROWS, 128), jnp.float32),
            pltpu.VMEM((5, 2, ROWS, 128), jnp.float32),
            pltpu.VMEM((16, 2 * LATTICE + 5, 8, 128), jnp.float32),
            pltpu.VMEM((128, 128), jnp.float32),
            pltpu.VMEM((128, 128), jnp.float32),
            pltpu.VMEM((16, 4, 128), jnp.float32),
            pltpu.VMEM((16, 4, 128), jnp.float32),
            pltpu.SemaphoreType.DMA((4,)),
            pltpu.SemaphoreType.DMA((16,)),
            pltpu.SemaphoreType.DMA((16,)),
            pltpu.SemaphoreType.DMA((16,)),
            pltpu.SemaphoreType.DMA((16,)),
        ],
        compiler_params=pltpu.CompilerParams(
            collective_id=0, has_side_effects=True, vmem_limit_bytes=50 * 1024 * 1024
        ),
    )(*[pltpu.with_memory_space_constraint(value, pltpu.HBM) for value in arguments])
    return (lattice[None], water)


def solution(mesh):
    in_specs = (
        P("side", None, None, "gx", "gy"),
        P("side", None, "gx", "gy"),
        P(None, "gx", ("side", "gy")),
        P("gx", ("side", "gy")),
    )
    out_specs = (P("side", None, None, "gx", "gy"), P(None, "gx", ("side", "gy")))
    return jax.shard_map(
        on_device, mesh=mesh, in_specs=in_specs, out_specs=out_specs, check_vma=False
    )
```

```python
import functools

import jax
import jax.numpy as jnp
from jax import lax
from jax.experimental import pallas as pl
from jax.experimental.pallas import tpu as pltpu
from jax.sharding import PartitionSpec as P

STEPS = 8
SUBSTEPS = 2
LATTICE = 19
MESH = pl.DeviceIdType.MESH

velocity_table = (
    (0, 0, 0),
    (1, 0, 0),
    (-1, 0, 0),
    (0, 1, 0),
    (0, -1, 0),
    (0, 0, 1),
    (0, 0, -1),
    (1, 1, 0),
    (-1, -1, 0),
    (1, -1, 0),
    (-1, 1, 0),
    (1, 0, 1),
    (-1, 0, -1),
    (1, 0, -1),
    (-1, 0, 1),
    (0, 1, 1),
    (0, -1, -1),
    (0, 1, -1),
    (0, -1, 1),
)
opposite_index = (0, 2, 1, 4, 3, 6, 5, 8, 7, 10, 9, 12, 11, 14, 13, 16, 15, 18, 17)
weight_table = (1.0 / 3.0,) + (1.0 / 18.0,) * 6 + (1.0 / 36.0,) * 12
relax_time = 0.8
coupling = -3.0
wall_potential = 0.4
uptake_rate = 0.02
drag_rate = 0.03
base_diffusion = 0.05
slope_diffusion = 0.015

PAIRS = 10
PAD = 8
ROWS = 16 * PAIRS + 2 * PAD
MASK_PLANE = LATTICE
FLUX_PLANE = LATTICE + 1
PLANES = LATTICE + 2
RATE = 1.0 / relax_time
KAPPA = RATE / 36.0


def roll(values, shift):
    shift = shift % 128
    if shift == 0:
        return values
    return pltpu.roll(values, shift, values.ndim - 1)


def lanes_of(shape):
    return lax.broadcasted_iota(jnp.int32, shape, len(shape) - 1)


def uptake(density_row):
    activity = density_row / (1.0 + density_row)
    return 0.043 + activity * (17.18 + activity * (-39.85 + 36.0 * activity))


def pack_columns(ref, offset, rows):
    lanes = lanes_of((rows, 128))
    packed = None
    for m in range(4):
        part = roll(ref[pl.ds(m, rows, stride=4), :], 32 * m - offset)
        packed = part if packed is None else jnp.where(lanes >= 32 * m, part, packed)
    return packed


def unpack_columns(packed, ref):
    for m in range(4):
        ref[pl.ds(m, packed.shape[0], stride=4), :] = roll(packed, -32 * m)


def pack_pair(a, b):
    lower = lanes_of(a.shape) % 32 < 16
    return jnp.where(lower, a, roll(b, 16)), jnp.where(lower, roll(a, -16), b)


def sheet_update(water_ref, current_ref, surface_ref, sheet_ref):
    depth = water_ref.shape[0]

    def rows_of(block, carry):
        rows = pl.ds(pl.multiple_of(block * 8, 8), 8)
        surfaces = surface_ref[rows, :]
        water = [water_ref[k, rows, :] for k in range(depth)]
        drag = drag_rate * current_ref[rows, :]
        both = uptake(surfaces)
        inflow_anode = uptake_rate * (both[:, :64] - water[0])
        inflow_cathode = uptake_rate * (roll(both, 64)[:, :64] - water[depth - 1])
        for _ in range(SUBSTEPS):
            below = inflow_anode
            fresh = []
            for k in range(depth):
                if k < depth - 1:
                    mean = base_diffusion + (0.5 * slope_diffusion) * (water[k] + water[k + 1])
                    above = drag * water[k] - mean * (water[k + 1] - water[k])
                else:
                    above = -inflow_cathode
                fresh.append(water[k] + (below - above))
                below = above
            water = fresh
        for k in range(depth):
            sheet_ref[k, rows, :] = water[k]
        return carry

    lax.fori_loop(0, water_ref.shape[1] // 8, rows_of, 0)


def step_kernel(
    pop_hbm,
    mask_hbm,
    water_hbm,
    current_hbm,
    out_ref,
    sheet_ref,
    window,
    flux_window,
    raw_mask,
    water_ref,
    current_ref,
    own,
    pack_low,
    pack_high,
    halo_low,
    halo_high,
    fields_even,
    fields_odd,
    coefficients,
    flux,
    slopes,
    centres,
    stage,
    square,
    columns,
    send_pieces,
    recv_pieces,
    load_sem,
    send_sem,
    recv_sem,
    piece_send_sem,
    piece_recv_sem,
):
    side, gx, gy = lax.axis_index("side"), lax.axis_index("gx"), lax.axis_index("gy")
    gx_count, gy_count = lax.axis_size("gx"), lax.axis_size("gy")
    groups = 2 * gy_count
    me = side * gy_count + gy
    x_up = (side, lax.rem(gx + 1, gx_count), gy)
    x_down = (side, lax.rem(gx + gx_count - 1, gx_count), gy)
    y_up = (side, gx, lax.rem(gy + 1, gy_count))
    y_down = (side, gx, lax.rem(gy + gy_count - 1, gy_count))

    def peer(distance):
        other = lax.rem(me + distance, groups)
        return other, (other // gy_count, gx, lax.rem(other, gy_count))

    barrier = pltpu.get_barrier_semaphore()
    for device in [x_up, x_down] + [peer(d)[1] for d in range(1, groups)]:
        pl.semaphore_signal(barrier, inc=1, device_id=device, device_id_type=MESH)
    loads = [
        pltpu.make_async_copy(source, target, load_sem.at[k])
        for k, (source, target) in enumerate(
            ((pop_hbm, window.at[pl.ds(0, LATTICE), :, :, pl.ds(16, 32), :]), (mask_hbm, raw_mask), (water_hbm, water_ref), (current_hbm, current_ref))
        )
    ]
    for load in loads:
        load.start()

    copies = []

    def prepare(src, dst, device):
        slot = len(copies)
        copy = pltpu.make_async_remote_copy(
            src_ref=src,
            dst_ref=dst,
            send_sem=send_sem.at[slot],
            recv_sem=recv_sem.at[slot],
            device_id=device,
            device_id_type=MESH,
        )
        copies.append(copy)
        return copy

    def send(src, dst, device):
        copy = prepare(src, dst, device)
        copy.start()
        return copy

    loads[0].wait()
    pl.semaphore_wait(barrier, groups + 1)

    lattice = pl.ds(0, LATTICE)
    edges = ((16, 48, x_down), (32, 0, x_up))
    x_copies = [
        send(
            window.at[lattice, :, :, pl.ds(source, 16), :], window.at[lattice, :, :, pl.ds(target, 16), :], device
        )
        for source, target, device in edges
    ]
    loads[1].wait()
    window[MASK_PLANE, :, :, 16:48, :] = raw_mask[...].astype(jnp.float32)
    x_copies += [
        send(
            window.at[MASK_PLANE, :, :, pl.ds(source, 16), :],
            window.at[MASK_PLANE, :, :, pl.ds(target, 16), :],
            device,
        )
        for source, target, device in edges
    ]

    loads[2].wait()
    loads[3].wait()
    square[0:32, 0:64] = water_ref[0]
    square[32:64, 0:64] = water_ref[water_ref.shape[0] - 1]
    columns[...] = jnp.swapaxes(square[...], 0, 1)
    for s in range(2):
        faces = pack_columns(columns.at[pl.ds(0, 64)], 32 * s, 16)
        for g in range(8):
            send_pieces[s * 8 + g, 2:4, :] = faces[2 * g : 2 * g + 2]
    total = None
    for i in range(LATTICE):
        part = window[i, 0, 0, 16:48, :]
        total = part if total is None else total + part
    square[0:32, :] = total
    columns[...] = jnp.swapaxes(square[...], 0, 1)
    surface = pack_columns(columns, 0, 32)
    for c in range(16):
        send_pieces[c, 0:2, :] = surface[2 * c : 2 * c + 2]
    pieces = []
    for d in range(1, groups):
        other, device = peer(d)
        copy = pltpu.make_async_remote_copy(
            src_ref=send_pieces.at[other],
            dst_ref=recv_pieces.at[me],
            send_sem=piece_send_sem.at[d],
            recv_sem=piece_recv_sem.at[d],
            device_id=device,
            device_id_type=MESH,
        )
        copy.start()
        pieces.append(copy)

    for i in range(LATTICE + 1):
        turned = jnp.swapaxes(window[i, :, :, 16:48, :].reshape(128, 128), 0, 1)
        own[i, 1] = turned[0:16].reshape(2, 8, 128)
        own[i, 8] = turned[112:128].reshape(2, 8, 128)
    main = pl.ds(0, LATTICE + 1)
    y_copies = [
        send(own.at[main, 8], own.at[main, 0], y_up),
        send(own.at[main, 1], own.at[main, 9], y_down),
    ]

    lane = lanes_of((8, 128))
    first = lane < 64
    last = lane >= 64
    is_low = lane % 64 < 16
    is_high = lane % 64 >= 48

    def planes_at(t, planes):
        start = pl.multiple_of(t * 16 + PAD, 8)
        for i in planes:
            for k in range(2):
                rows = pl.ds(start + 8 * k, 8)
                if i < LATTICE:
                    moved = pl.ds(start + 8 * k - velocity_table[i][1], 8)
                    yield i, k, [fields_even.at[0, i, g, moved, :] for g in range(2)]
                elif i == MASK_PLANE:
                    yield i, k, [coefficients.at[0, g, rows, :] for g in range(2)]
                else:
                    yield i, k, [flux.at[rows, :], None]

    def set_coefficients(g, rows, pore):
        coefficients[0, g, rows, :] = pore
        coefficients[1, g, rows, :] = (3.0 * KAPPA) * pore
        coefficients[2, g, rows, :] = (0.5 + 0.5 * (RATE - 1.0)) * pore - 0.5
        coefficients[3, g, rows, :] = 0.5 - (0.5 - 0.5 * (RATE - 1.0)) * pore
        coefficients[4, g, rows, :] = 1.0 - RATE * pore

    def place_own(t, planes):
        for i, k, targets in planes_at(t, planes):
            tile = own[i, t, k]
            for target, shift in zip(targets, (16, -16)):
                if target is not None:
                    target[...] = roll(tile, shift)

    def place_halo(t, planes):
        for i, k, targets in planes_at(t, planes):
            low, high = halo_low[i, t // 9], halo_high[i, t // 9]
            for g, target in enumerate(targets):
                if target is not None:
                    pltpu.store(target, roll(low, -16 * k - 32 * g), mask=is_low)
                    pltpu.store(target, roll(high, 48 - 16 * k - 32 * g), mask=is_high)
        start = pl.multiple_of(t * 16 + PAD, 8)
        for k in range(2):
            rows = pl.ds(start + 8 * k, 8)
            for g in range(2):
                set_coefficients(g, rows, coefficients[0, g, rows, :])

    recv_pieces[me] = send_pieces[me]
    for copy in pieces:
        copy.wait()
    for c in range(16):
        square[2 * c : 2 * c + 2, :] = recv_pieces[c, 2:4, :]
        square[32 + 2 * c : 34 + 2 * c, :] = recv_pieces[c, 0:2, :]
    own_surface = columns[...]
    unpack_columns(square[0:32, :], columns)
    own_inflow = uptake_rate * (uptake(own_surface) - columns[...])
    own[FLUX_PLANE, 1] = own_inflow[0:16].reshape(2, 8, 128)
    own[FLUX_PLANE, 8] = own_inflow[112:128].reshape(2, 8, 128)
    flux_window[16:48, :] = jnp.swapaxes(own_inflow, 0, 1)[0:32]
    y_copies += [
        send(own.at[FLUX_PLANE, 8], own.at[FLUX_PLANE, 0], y_up),
        send(own.at[FLUX_PLANE, 1], own.at[FLUX_PLANE, 9], y_down),
    ]
    x_copies += [
        send(flux_window.at[pl.ds(source, 16), :], flux_window.at[pl.ds(target, 16), :], device)
        for source, target, device in edges
    ]
    unpack_columns(square[32:64, :], columns)
    square[...] = jnp.swapaxes(columns[...], 0, 1)
    sheet_update(water_ref, current_ref, square, sheet_ref)

    corner_copies = []
    for end in range(2):
        corner_copies += [
            prepare(pack_low.at[:, end], halo_high.at[:, end], x_down),
            prepare(pack_high.at[:, end], halo_low.at[:, end], x_up),
        ]

    def pack_corners(k, carry):
        for i in range(3):
            for t in (0, 9):
                low, high = pack_pair(own[3 * k + i, t, 0], own[3 * k + i, t, 1])
                pack_low[3 * k + i, t // 9] = low
                pack_high[3 * k + i, t // 9] = high
        return carry

    def pass_corners():
        for copy in y_copies:
            copy.wait()
        lax.fori_loop(0, PLANES // 3, pack_corners, 0)
        for copy in corner_copies:
            copy.start()
        for t in (0, 9):
            place_own(t, range(PLANES))

    zero = jnp.zeros((8, 128), jnp.float32)

    def layers_sum(a, b, a_turned, b_turned):
        return b + jnp.where(last, b_turned, zero), a + jnp.where(first, a_turned, zero)

    def layers_difference(a, b, a_turned, b_turned):
        return b - jnp.where(last, b_turned, zero), jnp.where(first, a_turned, zero) - a

    def load_fields(fields, group, start):
        return [
            fields[i, group, pl.ds(start - velocity_table[i][1], 8), :] for i in range(LATTICE)
        ]

    def potentials(fields, slopes, start):
        rows = pl.ds(start, 8)
        potential = []
        for g in range(2):
            loaded = load_fields(fields, g, start)
            while len(loaded) > 1:
                loaded = [
                    loaded[k] + loaded[k + 1] if k + 1 < len(loaded) else loaded[k]
                    for k in range(0, len(loaded), 2)
                ]
            rho = loaded[0]
            pore = coefficients[0, g, rows, :]
            is_pore = pore > 0.5
            value = jnp.where(is_pore, 1.0 - jnp.exp(-rho), wall_potential)
            potential.append(value)
            centres[0, g, rows, :] = (KAPPA * pore) * rho
            centres[1, g, rows, :] = (0.5 / KAPPA) / rho
            centres[2, g, rows, :] = (3.0 * KAPPA * relax_time * -coupling / 36.0) * (pore * value)
        right = [roll(p, -1) for p in potential]
        left = [roll(p, 1) for p in potential]
        turned = [roll(p, 64) for p in potential]
        right_turned = [roll(p, 63) for p in potential]
        left_turned = [roll(p, 65) for p in potential]
        slope_x = [right[g] - left[g] for g in range(2)]
        slope_x_turned = [right_turned[g] - left_turned[g] for g in range(2)]
        wide = [(potential[g] + potential[g]) + (right[g] + left[g]) for g in range(2)]
        wide_turned = [(turned[g] + turned[g]) + (right_turned[g] + left_turned[g]) for g in range(2)]
        layers = layers_sum(*potential, *turned)
        slope_z = layers_difference(*potential, *turned)
        slope_x_layers = layers_sum(*slope_x, *slope_x_turned)
        slope_z_wide = layers_difference(*wide, *wide_turned)
        for g in range(2):
            slopes[0, g, rows, :] = slope_x[g]
            slopes[1, g, rows, :] = wide[g] + layers[g]
            slopes[2, g, rows, :] = slope_z[g]
            centres[3, g, rows, :] = (slope_x[g] + slope_x[g]) + slope_x_layers[g]
            centres[4, g, rows, :] = slope_z_wide[g]

    def collide(fields, slopes, g, start):
        rows = pl.ds(start, 8)
        above, below = pl.ds(start + 1, 8), pl.ds(start - 1, 8)
        f = load_fields(fields, g, start)
        odd = [None] + [f[i] - f[i + 1] for i in range(1, LATTICE, 2)]
        sums = [None] + [f[i] + f[i + 1] for i in range(1, LATTICE, 2)]
        moment = (
            (odd[1] + odd[4]) + (odd[5] + (odd[6] + odd[7])),
            (odd[2] + odd[4]) + ((odd[8] + odd[9]) - odd[5]),
            (odd[3] + odd[6]) + ((odd[8] - odd[9]) - odd[7]),
        )
        gradient = (
            centres[3, g, rows, :] + (slopes[0, g, above, :] + slopes[0, g, below, :]),
            slopes[1, g, above, :] - slopes[1, g, below, :],
            centres[4, g, rows, :] + (slopes[2, g, above, :] + slopes[2, g, below, :]),
        )
        factor = centres[2, g, rows, :]
        three = coefficients[1, g, rows, :]
        even_part = coefficients[2, g, rows, :]
        odd_part = coefficients[3, g, rows, :]
        flow = [three * moment[c] + factor * gradient[c] for c in range(3)]
        speed = flow[0] * flow[0] + flow[1] * flow[1] + flow[2] * flow[2]
        scaled = centres[1, g, rows, :]
        base = centres[0, g, rows, :] - (1.0 / 3.0) * (speed * scaled)
        double = base + base
        post = [None] * LATTICE
        post[0] = 12.0 * base + coefficients[4, g, rows, :] * f[0]
        for p in range(1, 10):
            i = 2 * p - 1
            velocity = velocity_table[i]
            along = None
            for c in range(3):
                if velocity[c] == 0:
                    continue
                if along is None:
                    along = flow[c]
                elif velocity[c] > 0:
                    along = along + flow[c]
                else:
                    along = along - flow[c]
            if i < 7:
                twice = along + along
                even = double + twice * (along * scaled)
                along = twice
            else:
                even = base + along * (along * scaled)
            even = even - even_part * sums[p]
            along = along - odd_part * odd[p]
            post[i] = even + along
            post[i + 1] = even - along
        return post

    def relax(fields, slopes, start, half):
        a = collide(fields, slopes, 0, start)
        b = collide(fields, slopes, 1, start)
        wall_flux = flux[pl.ds(start, 8), :]
        walls = 0
        for i in range(LATTICE):
            stage[half, i] = a[i]
            stage[half, LATTICE + i] = b[i]
            if velocity_table[i][2] == 1:
                stage[half, 2 * LATTICE + walls] = (
                    a[opposite_index[i]] - (6.0 * weight_table[i]) * wall_flux
                )
                walls += 1

    def move(fields, start, half):
        rows = pl.ds(start, 8)
        walls = 0
        for i in range(LATTICE):
            shift_x, shift_y, shift_z = velocity_table[i]
            moved = pl.ds(start - shift_y, 8)
            a, b = stage[half, i], stage[half, LATTICE + i]
            if shift_z == 0:
                fields[i, 0, rows, :] = roll(a, shift_x)
                fields[i, 1, rows, :] = roll(b, shift_x)
            elif shift_z == 1:
                fields[i, 1, rows, :] = roll(a, shift_x)
                pltpu.store(fields.at[i, 0, rows, :], roll(b, 64 + shift_x), mask=last)
                wall = stage[half, 2 * LATTICE + walls]
                pltpu.store(fields.at[i, 0, moved, :], wall, mask=first)
                walls += 1
            else:
                fields[i, 0, rows, :] = roll(b, shift_x)
                pltpu.store(fields.at[i, 1, rows, :], roll(a, 64 + shift_x), mask=first)
                wall = stage[half, LATTICE + opposite_index[i]]
                pltpu.store(fields.at[i, 1, moved, :], wall, mask=last)

    def run_steps(tiles, begin, end, after_two=None):
        starts = [tile * 8 + PAD for tile in tiles]

        def one_step(step, now, then):
            for start in starts:
                potentials(now, slopes.at[step], start)
            for slot, start in enumerate(starts):
                relax(now, slopes.at[step], start, slot)
                if slot % 2 == 1 and slot > 2:
                    for done in (slot - 3, slot - 2):
                        move(then, starts[done], done)
            for done in (len(starts) - 2, len(starts) - 1):
                move(then, starts[done], done)

        def two_steps(half, carry):
            one_step(2 * half, fields_even.at[half], fields_odd.at[half])
            one_step(2 * half + 1, fields_odd.at[half], fields_even.at[half + 1])
            if after_two is not None:
                pl.when(half == begin // 2)(after_two)
            return carry

        lax.fori_loop(begin // 2, end // 2, two_steps, 0)

    for copy in x_copies[:4]:
        copy.wait()
    for i in range(LATTICE + 1):
        for g in range(2):
            turned = jnp.swapaxes(window[i, :, g].reshape(128, 128), 0, 1)
            if i < LATTICE:
                fields_even[0, i, g, pl.ds(PAD + 16 - velocity_table[i][1], 128), :] = turned
            else:
                set_coefficients(g, pl.ds(PAD + 16, 128), turned)
    for copy in x_copies[4:]:
        copy.wait()
    flux[pl.ds(PAD + 16, 128), :] = jnp.swapaxes(flux_window[...], 0, 1)
    run_steps(range(2, 18), 0, STEPS, pass_corners)
    for copy in corner_copies:
        copy.wait()
    for t in (0, 9):
        place_halo(t, range(PLANES))
    for base in range(2):
        ends = [base + k for k in range(3)] + [17 - base + k for k in range(3)]
        run_steps(ends, base * STEPS // 2, (base + 1) * STEPS // 2)

    for i in range(LATTICE):
        rows = pl.ds(PAD + 16 - velocity_table[i][1], 128)
        for g in range(2):
            turned = jnp.swapaxes(fields_even[STEPS // 2, i, g, rows, :], 0, 1)
            out_ref[i, g] = turned[16:48]
            out_ref[i, g + 2] = turned[80:112]


def on_device(populations, solid_mask, water_sheet, current):
    arguments = (
        populations.reshape(LATTICE, 2, 2, 32, 128),
        solid_mask.reshape(2, 2, 32, 128),
        water_sheet,
        current,
    )
    vmem = pl.BlockSpec(memory_space=pltpu.VMEM)
    hbm = pl.BlockSpec(memory_space=pltpu.HBM)
    lattice, water = pl.pallas_call(
        step_kernel,
        out_shape=(
            jax.ShapeDtypeStruct(populations.shape[1:], jnp.float32),
            jax.ShapeDtypeStruct(water_sheet.shape, jnp.float32),
        ),
        in_specs=[hbm, hbm, hbm, hbm],
        out_specs=(vmem, vmem),
        scratch_shapes=[
            pltpu.VMEM((LATTICE + 1, 2, 2, 64, 128), jnp.float32),
            pltpu.VMEM((128, 128), jnp.float32),
            pltpu.VMEM((2, 2, 32, 128), jnp.int32),
            pltpu.VMEM(water_sheet.shape, jnp.float32),
            pltpu.VMEM(current.shape, jnp.float32),
            pltpu.VMEM((PLANES, PAIRS, 2, 8, 128), jnp.float32),
            pltpu.VMEM((PLANES, 2, 8, 128), jnp.float32),
            pltpu.VMEM((PLANES, 2, 8, 128), jnp.float32),
            pltpu.VMEM((PLANES, 2, 8, 128), jnp.float32),
            pltpu.VMEM((PLANES, 2, 8, 128), jnp.float32),
            pltpu.VMEM((STEPS // 2 + 1, LATTICE, 2, ROWS, 128), jnp.float32),
            pltpu.VMEM((STEPS // 2, LATTICE, 2, ROWS, 128), jnp.float32),
            pltpu.VMEM((5, 2, ROWS, 128), jnp.float32),
            pltpu.VMEM((ROWS, 128), jnp.float32),
            pltpu.VMEM((STEPS, 3, 2, ROWS, 128), jnp.float32),
            pltpu.VMEM((5, 2, ROWS, 128), jnp.float32),
            pltpu.VMEM((16, 2 * LATTICE + 5, 8, 128), jnp.float32),
            pltpu.VMEM((128, 128), jnp.float32),
            pltpu.VMEM((128, 128), jnp.float32),
            pltpu.VMEM((16, 4, 128), jnp.float32),
            pltpu.VMEM((16, 4, 128), jnp.float32),
            pltpu.SemaphoreType.DMA((4,)),
            pltpu.SemaphoreType.DMA((16,)),
            pltpu.SemaphoreType.DMA((16,)),
            pltpu.SemaphoreType.DMA((16,)),
            pltpu.SemaphoreType.DMA((16,)),
        ],
        compiler_params=pltpu.CompilerParams(
            collective_id=0, has_side_effects=True, vmem_limit_bytes=50 * 1024 * 1024
        ),
    )(*[pltpu.with_memory_space_constraint(value, pltpu.HBM) for value in arguments])
    return (lattice[None], water)


def solution(mesh):
    in_specs = (
        P("side", None, None, "gx", "gy"),
        P("side", None, "gx", "gy"),
        P(None, "gx", ("side", "gy")),
        P("gx", ("side", "gy")),
    )
    out_specs = (P("side", None, None, "gx", "gy"), P(None, "gx", ("side", "gy")))
    return jax.shard_map(
        on_device, mesh=mesh, in_specs=in_specs, out_specs=out_specs, check_vma=False
    )
```
